256 devices in a mesh: row: 16 (over x_hi, z), col: 16 (over y, x_lo, core).
Axes of the slice: x: 4 (x_hi: 2, x_lo: 2; x = x_hi * 2 + x_lo), y: 4, z: 8, core: 2. Of those that a mesh axis runs over, the one named last changes fastest.
Arguments:
- tile_values: float32 [16, 16, 16, 128, 128], P('row', 'col'), may hold values from -0.1875 to 0.1875
- tile_rows: int32 [16, 16, 16], P('row', 'col'), may hold values from 0 to 15, as said below
- tile_cols: int32 [16, 16, 16], P('row', 'col'), may hold values from 0 to 63
- tile_live: int32 [16, 16, 16], P('row', 'col'), may hold values from 0 to 1, as said below
- dense_factor: float32 [512, 131072], P('row', 'col'), may hold values from -6 to 6
Outputs:
- product_transposed: float32 [512, 32768], P('col', 'row')
The draws below stay inside these ranges and needn't reach their ends.
Inputs may be any that keep to these rules, and one draw needn't show every extreme that they name: `tile_rows`: tile row inside the block; the live tiles of one block have distinct (row, column) pairs. `tile_live`: in every block the live slots come first; the blocks (r, c) with |r − c| ≤ 1 have all 16 slots live; every other block has between 1 and 8 live slots.
All inputs are finite; a program needn't handle non-finite values.
Results may differ from the reference program's by a relative error of at most 0.0003.
Values sent between devices are 32-bit elements; how exact they have to be, the bound alone decides.
A program may use at most 64 MiB of HBM per device.

```python
import jax
import jax.numpy as jnp
from jax import lax

TS = 128
W = 512
RT = 16
CT = 64
MAXT = 16
GR = 16
GC = 16
N = 131072


def tile_pattern(key):
    base = jax.random.fold_in(key, 7101)
    first_key, second_key = jax.random.split(base, 2)
    slot_total = RT * CT
    scores = jax.random.randint(first_key, (GR, GC, slot_total), 0, 2 ** 30 // slot_total)
    scores = scores * slot_total + jnp.arange(slot_total, dtype=jnp.int32)
    order = jnp.argsort(scores, axis=-1, stable=True)[..., :MAXT].astype(jnp.int32)
    grid_row = jnp.arange(GR, dtype=jnp.int32)[:, None]
    grid_col = jnp.arange(GC, dtype=jnp.int32)[None, :]
    banded = jnp.abs(grid_row * GC - grid_col * GR) <= max(GR, GC)
    sparse_count = jax.random.randint(second_key, (GR, GC), 1, MAXT // 2 + 1)
    counts = jnp.where(banded, MAXT, sparse_count).astype(jnp.int32)
    live_mask = (jnp.arange(MAXT, dtype=jnp.int32)[None, None, :] < counts[..., None]).astype(jnp.int32)
    return (order // CT, order % CT, live_mask)


def draw_tile_rows(key, part):
    return tile_pattern(key)[0]


def draw_tile_cols(key, part):
    return tile_pattern(key)[1]


def draw_tile_live(key, part):
    return tile_pattern(key)[2]


def with_spikes(array, key, source, target, parts, factor):
    owner, partner = [(jnp.arange(array.shape[position]) // (array.shape[position] // parts)).reshape([-1 if axis == position else 1 for axis in range(array.ndim)]) for position in (source, target)]
    chosen = jax.random.permutation(key, parts)[partner]
    strong = (owner == chosen) | (owner == (partner + parts // 2) % parts)
    return jnp.where(strong, factor * array, array)


def block_scale(rng, extent, cuts, least, high):
    factor_of = 1.0
    for dim, shards_of in cuts:
        heights = jax.random.uniform(jax.random.fold_in(jax.random.fold_in(rng, 6), dim), (shards_of,), jnp.float32, least / len(cuts), high / len(cuts))
        factor_of = factor_of * jnp.repeat(jnp.exp(heights), extent[dim] // shards_of).reshape((-1,) + (1,) * (len(extent) - 1 - dim))
    return factor_of


def noise(key, dims, scale, reach, cuts=(), kind=jnp.bfloat16):
    loudness = block_scale(key, dims, cuts, -0.22, 0.18) if cuts else 1.0
    values = jax.random.normal(key, dims, jnp.float32) * scale * loudness
    return jnp.minimum(jnp.maximum(values, -reach), reach).astype(kind)


def noise_with(key, shape, spread, bound, cuts, heavy, kind=jnp.bfloat16):
    array = spread * jax.random.normal(key, shape, jnp.float32)
    if cuts:
        array = array * block_scale(key, shape, cuts, -0.22, 0.18)
    return jnp.clip(with_spikes(array, jax.random.fold_in(key, 3), *heavy), -bound, bound).astype(kind)


def setup_inputs(seed: int = 0) -> dict:
    seeds = jax.random.split(jax.random.key(seed), 6)
    tile_values = noise(seeds[0], (GR, GC, MAXT, TS, TS), (8 * TS) ** -0.5, 0.1875, ((0, 16), (1, 16)), jnp.float32)
    tile_rows = draw_tile_rows(jax.random.fold_in(seeds[5], 71), 0)
    tile_cols = draw_tile_cols(jax.random.fold_in(seeds[5], 71), 0)
    tile_live = draw_tile_live(jax.random.fold_in(seeds[5], 71), 0)
    dense_factor = noise_with(seeds[4], (W, N), 1.0, 6.0, ((0, 16), (1, 16)), (1, 0, 16, 2.0), jnp.float32)
    return dict(tile_values=tile_values, tile_rows=tile_rows, tile_cols=tile_cols, tile_live=tile_live, dense_factor=dense_factor)


def reference(tile_values, tile_rows, tile_cols, tile_live, dense_factor):
    grid_rows = tile_values.shape[0]
    grid_cols = tile_values.shape[1]
    slot_count = tile_values.shape[2]
    tile_size = tile_values.shape[3]
    width = dense_factor.shape[0]
    panels = dense_factor.reshape(width, grid_cols, CT, tile_size)
    row_tiles = jnp.arange(RT, dtype=jnp.int32)

    def block_step(running, flat_index):
        grid_row = flat_index // grid_cols
        grid_col = flat_index % grid_cols
        live_mask = tile_live[grid_row, grid_col].astype(jnp.float32)
        masked = tile_values[grid_row, grid_col] * live_mask[:, None, None]
        col_ids = tile_cols[grid_row, grid_col]
        row_ids = tile_rows[grid_row, grid_col]
        panel = lax.dynamic_index_in_dim(panels, grid_col, 1, keepdims=False)
        selected = jnp.take(panel, col_ids, axis=1)
        product = jnp.einsum("wsk,sik->wsi", selected, masked, precision=lax.Precision.HIGHEST)
        onehot = (row_ids[:, None] == row_tiles[None, :]).astype(jnp.float32)
        placed = jnp.einsum("wsi,sr->wri", product, onehot, precision=lax.Precision.HIGHEST)
        placed = placed.reshape(width, RT * tile_size)
        offset = (grid_row * (RT * tile_size)).astype(jnp.int32)
        previous = lax.dynamic_slice_in_dim(running, offset, RT * tile_size, 1)
        running = lax.dynamic_update_slice_in_dim(running, previous + placed, offset, 1)
        return running, None

    initial = jnp.zeros((width, grid_rows * RT * tile_size), jnp.float32)
    flat = jnp.arange(grid_rows * grid_cols, dtype=jnp.int32)
    result, unused = lax.scan(block_step, initial, flat)
    return result
```

```python
import jax
import jax.numpy as jnp
from jax import lax
from jax.experimental import pallas as pl
from jax.experimental.pallas import tpu as pltpu
from jax.sharding import PartitionSpec as P

NX, NY, NZ = 4, 4, 8
TS = 128
SHARE = 32
RT = 16
CT = 64
SLOTS = 16
PER = 2
CHUNKS = SLOTS // PER
HALF = CHUNKS // 2
PIECES = 4
SPAN = CT * TS // (2 * PIECES)
MESH = pl.DeviceIdType.MESH


def rem(a, b):
    return lax.rem(a, jnp.int32(b))


def div(a, b):
    return lax.div(a, jnp.int32(b))


def kernel(
    tiles, listed, dense, out,
    held, lists, lists_s, relay, both, split, acc, near, far, pair, done,
    local_sem, right_send, right_recv, left_send, left_recv,
    hop1_send, hop1_recv, hop2_send, hop2_recv, list_send, list_recv,
    near_send, near_recv, far_send, far_recv, pair_send, pair_recv, out_send, out_recv,
):
    row, col = lax.axis_index("row"), lax.axis_index("col")
    x_hi, z = div(row, NZ), rem(row, NZ)
    y, x_lo, core = div(col, 4), rem(div(col, 2), 2), rem(col, 2)
    x = x_hi * 2 + x_lo

    def device(x, y, z, core):
        return (div(x, 2) * NZ + z, y * 4 + rem(x, 2) * 2 + core)

    def copy(src, dst, send_sem, recv_sem, target):
        return pltpu.make_async_remote_copy(
            src_ref=src, dst_ref=dst, send_sem=send_sem, recv_sem=recv_sem,
            device_id=target, device_id_type=MESH,
        )

    up = device(x, y, rem(z + 1, NZ), core)
    down = device(x, y, rem(z + NZ - 1, NZ), core)

    def banded(source):
        gap = x_hi * NZ + source - col
        return jnp.logical_and(gap >= -1, gap <= 1)

    def ring(level, j, rightwards):
        if rightwards:
            source = rem(z + NZ - level, NZ)
        else:
            source = rem(z + level, NZ)
        part = held.at[source, pl.ds(PER * j, PER)]
        return source, part

    def listed_part(source, j, level, rightwards):
        there = jnp.logical_or(j < HALF, banded(source))
        if level == 3:
            first = rem(j, HALF) < HALF // 2
            there = jnp.logical_and(there, first if rightwards else jnp.logical_not(first))
        return there

    def ring_copy(level, j, rightwards):
        source, part = ring(level, j, rightwards)
        if rightwards:
            made = copy(part, part, right_send.at[level, j], right_recv.at[level, j], up)
        else:
            made = copy(part, part, left_send.at[level, j], left_recv.at[level, j], down)
        return listed_part(source, j, level, rightwards), made

    def ring_arrival(level, j, rightwards):
        source, part = ring(level + 1, j, rightwards)
        if rightwards:
            made = copy(part, part, right_send.at[level, j], right_recv.at[level, j], up)
        else:
            made = copy(part, part, left_send.at[level, j], left_recv.at[level, j], down)
        return listed_part(source, j, level, rightwards), made

    def ring_start(level, j):
        for rightwards in (True, False):
            there, made = ring_copy(level, j, rightwards)
            pl.when(there)(made.start)

    def ring_wait(level, j):
        for rightwards in (True, False):
            there, made = ring_arrival(level, j, rightwards)
            pl.when(there)(made.wait_recv)

    forth = device(rem(x + 1, NX), y, z, core)
    back = device(rem(x + NX - 1, NX), y, z, core)

    def columns(way, k):
        return pl.ds(pl.multiple_of((way * PIECES + k) * SPAN, SPAN), SPAN)

    def hop1(way, k):
        return copy(
            both.at[x_hi, :, columns(way, k)], relay.at[way, k],
            hop1_send.at[way, k], hop1_recv.at[way, k], (forth, back)[way],
        )

    def hop2(way, k):
        origin = div(rem(x + (NX - 1 if way == 0 else 1), NX), 2)
        return copy(
            relay.at[way, k], both.at[origin, :, columns(way, k)],
            hop2_send.at[way, k], hop2_recv.at[way, k], (forth, back)[way],
        )

    def hop2_arrival(way, k):
        return copy(
            relay.at[way, k], both.at[1 - x_hi, :, columns(way, k)],
            hop2_send.at[way, k], hop2_recv.at[way, k], (forth, back)[way],
        )

    def list_copy(p):
        target = device(x, y, rem(z + p, NZ), core)
        return copy(lists.at[z], lists.at[z], list_send.at[p], list_recv.at[z], target)

    def list_arrival(p):
        source = rem(z + p, NZ)
        target = device(x, y, source, core)
        return copy(lists.at[source], lists.at[source], list_send.at[p], list_recv.at[source], target)

    own_dense = pltpu.make_async_copy(dense, both.at[x_hi], local_sem.at[0])
    own_tiles = pltpu.make_async_copy(tiles, held.at[z], local_sem.at[1])
    own_list = pltpu.make_async_copy(listed, lists.at[z], local_sem.at[2])
    own_list.start()
    own_tiles.start()
    own_dense.start()
    own_list.wait()

    @pl.loop(1, NZ)
    def _(p):
        list_copy(p).start()

    own_tiles.wait()

    @pl.loop(0, CHUNKS)
    def _(j):
        ring_start(0, j)

    own_dense.wait()

    @pl.loop(0, PIECES)
    def _(k):
        hop1(0, k).start()
        hop1(1, k).start()

    @pl.loop(0, NZ * RT)
    def _(i):
        acc[div(i, RT), rem(i, RT)] = jnp.zeros((2 * SHARE, TS), jnp.float32)

    def one_tile(b, slot):
        tile = held[b, slot]
        high = tile.astype(jnp.bfloat16)
        low = (tile - high.astype(jnp.float32)).astype(jnp.bfloat16)
        chosen = split[lists_s[b, 1, slot]]
        dims = (((1,), (1,)), ((), ()))
        by_high = lax.dot_general(chosen, high, dims, preferred_element_type=jnp.float32)
        by_low = lax.dot_general(
            chosen[: 2 * SHARE], low, dims, preferred_element_type=jnp.float32
        )
        return by_high[: 2 * SHARE] + (by_high[2 * SHARE :] + by_low)

    def multiply(b, j):
        @pl.when(jnp.logical_or(j < HALF, banded(b)))
        def _():
            products = [one_tile(b, PER * j + s) for s in range(PER)]
            for k in range(RT):
                term = acc[b, k]
                for s in range(PER):
                    slot = PER * j + s
                    live = lists_s[b, 2, slot].astype(jnp.float32)
                    weight = jnp.where(lists_s[b, 0, slot] == k, live, 0.0)
                    term = term + weight * products[s]
                acc[b, k] = term

    def near_copy(b):
        return copy(
            acc.at[b, pl.ds((1 - core) * 8, 8)], near.at[b],
            near_send.at[b], near_recv.at[b], device(x, y, z, 1 - core),
        )

    def far_copy(b, step):
        there = rem(y + step, NY)
        return copy(
            acc.at[b, pl.ds(core * 8 + there * 2, 2)], far.at[b, step - 1],
            far_send.at[b, step - 1], far_recv.at[b, step - 1], device(x, there, z, core),
        )

    def pair_copy(b):
        return copy(
            acc.at[b, core * 8 + y * 2 + (1 - x_lo)], pair.at[b],
            pair_send.at[b], pair_recv.at[b], device(x_hi * 2 + 1 - x_lo, y, z, core),
        )

    mine = core * 8 + y * 2 + x_lo

    def out_copy(b, a):
        return copy(
            done.at[b, pl.ds(a * SHARE, SHARE)], out.at[:, pl.ds(pl.multiple_of(mine * TS, TS), TS)],
            out_send.at[b, a], out_recv.at[mine], (x_hi * NZ + b, a * NZ + z),
        )

    def stage1(b):
        near_copy(b).start()

    def stage2(b):
        near_copy(b).wait_recv()

        @pl.loop(0, 8)
        def _(k):
            acc[b, core * 8 + k] = acc[b, core * 8 + k] + near[b, k]

        for step in (1, 2, 3):
            far_copy(b, step).start()

    def stage3(b):
        for step in (1, 2, 3):
            far_copy(b, step).wait_recv()
        for k in range(2):
            place = core * 8 + y * 2 + k
            acc[b, place] = acc[b, place] + (far[b, 0, k] + far[b, 1, k] + far[b, 2, k])
        pair_copy(b).start()

    def is_home(b, a):
        return jnp.logical_and(b == z, a * NZ + z == col)

    def stage4(b):
        pair_copy(b).wait_recv()
        done[b] = acc[b, mine] + pair[b]
        for a in range(2):
            home = is_home(b, a)

            @pl.when(home)
            def _():
                out[:, pl.ds(pl.multiple_of(mine * TS, TS), TS)] = done[b, a * SHARE : (a + 1) * SHARE]

            @pl.when(jnp.logical_not(home))
            def _():
                out_copy(b, a).start()

    @pl.loop(0, CHUNKS)
    def _(j):
        @pl.when(j < PIECES)
        def _():
            for way in (0, 1):
                hop1(way, j).wait_recv()
                hop2(way, j).start()

        ring_wait(0, j)
        ring_start(1, j)

    @pl.loop(0, CHUNKS)
    def _(j):
        ring_wait(1, j)
        ring_start(2, j)

    @pl.loop(1, NZ)
    def _(p):
        list_arrival(p).wait_recv()

    to_scalar = pltpu.make_async_copy(lists, lists_s, local_sem.at[3])
    to_scalar.start()

    @pl.loop(0, PIECES)
    def _(k):
        for way in (0, 1):
            hop2_arrival(way, k).wait_recv()

    @pl.loop(0, CT)
    def _(t):
        place = pl.ds(pl.multiple_of(t * TS, TS), TS)
        for a in range(2):
            value = both[a, :, place]
            high = value.astype(jnp.bfloat16)
            low = (value - high.astype(jnp.float32)).astype(jnp.bfloat16)
            split[t, a * SHARE : (a + 1) * SHARE] = high
            split[t, (2 + a) * SHARE : (3 + a) * SHARE] = low

    to_scalar.wait()

    def block(i):
        return rem(z + i + NZ, NZ)

    @pl.loop(0, CHUNKS)
    def _(j):
        ring_wait(2, j)
        ring_start(3, j)

        @pl.loop(0, 5)
        def _(i):
            multiply(block(i - 2), j)

    @pl.loop(0, 5)
    def _(i):
        stage1(block(i - 2))

    @pl.loop(0, CHUNKS)
    def _(j):
        for i in (-3, 3):
            multiply(block(i), j)

    stage1(block(-3))
    stage1(block(3))

    @pl.loop(0, 5)
    def _(i):
        stage2(block(i - 2))

    @pl.loop(0, CHUNKS)
    def _(j):
        ring_wait(3, j)
        multiply(block(4), j)

    stage1(block(4))

    @pl.loop(0, 5)
    def _(i):
        stage3(block(i - 2))

    stage2(block(-3))
    stage2(block(3))
    stage2(block(4))

    @pl.loop(0, 5)
    def _(i):
        stage4(block(i - 2))

    stage3(block(-3))
    stage3(block(3))
    stage3(block(4))
    stage4(block(-3))
    stage4(block(3))
    stage4(block(4))

    @pl.loop(0, RT)
    def _(t):
        source = (div(rem(t, 8), 2) * 2 + rem(t, 2)) * 2 + div(t, 8)
        there = out.at[:, pl.ds(pl.multiple_of(t * TS, TS), TS)]
        home = jnp.logical_and(source == col, rem(col, NZ) == z)

        @pl.when(jnp.logical_not(home))
        def _():
            copy(
                done.at[0, pl.ds(0, SHARE)], there, out_send.at[0, 0], out_recv.at[t],
                (row, rem(col + 1, 16)),
            ).wait_recv()

    @pl.loop(1, NZ)
    def _(p):
        list_copy(p).wait_send()

    @pl.loop(0, CHUNKS)
    def _(j):
        for level in range(4):
            for rightwards in (True, False):
                there, made = ring_copy(level, j, rightwards)
                pl.when(there)(made.wait_send)

    @pl.loop(0, PIECES)
    def _(k):
        for way in (0, 1):
            hop1(way, k).wait_send()
            hop2(way, k).wait_send()

    @pl.loop(0, NZ)
    def _(b):
        near_copy(b).wait_send()
        for step in (1, 2, 3):
            far_copy(b, step).wait_send()
        pair_copy(b).wait_send()
        for a in range(2):
            pl.when(jnp.logical_not(is_home(b, a)))(out_copy(b, a).wait_send)


def body(tile_values, tile_rows, tile_cols, tile_live, dense_factor):
    lists = jnp.concatenate(
        [tile_rows[0], tile_cols[0], tile_live[0], jnp.zeros((5, SLOTS), jnp.int32)], axis=0
    )
    lists = jnp.pad(lists, ((0, 0), (0, TS - SLOTS)))
    dma = pltpu.SemaphoreType.DMA
    vmem = pltpu.VMEM
    f32 = jnp.float32
    return pl.pallas_call(
        kernel,
        out_shape=jax.ShapeDtypeStruct((SHARE, RT * TS), f32),
        in_specs=[pl.BlockSpec(memory_space=pl.ANY)] * 3,
        out_specs=pl.BlockSpec(memory_space=pltpu.VMEM),
        scratch_shapes=[
            vmem((NZ, SLOTS, TS, TS), f32),
            vmem((NZ, 8, TS), jnp.int32),
            pltpu.SMEM((NZ, 8, TS), jnp.int32),
            vmem((2, PIECES, SHARE, SPAN), f32),
            vmem((2, SHARE, CT * TS), f32),
            vmem((CT, 4 * SHARE, TS), jnp.bfloat16),
            vmem((NZ, RT, 2 * SHARE, TS), f32),
            vmem((NZ, 8, 2 * SHARE, TS), f32),
            vmem((NZ, 3, 2, 2 * SHARE, TS), f32),
            vmem((NZ, 2 * SHARE, TS), f32),
            vmem((NZ, 2 * SHARE, TS), f32),
            dma((4,)),
            dma((4, CHUNKS)), dma((4, CHUNKS)), dma((4, CHUNKS)), dma((4, CHUNKS)),
            dma((2, PIECES)), dma((2, PIECES)), dma((2, PIECES)), dma((2, PIECES)),
            dma((NZ,)), dma((NZ,)),
            dma((NZ,)), dma((NZ,)), dma((NZ, 3)), dma((NZ, 3)), dma((NZ,)), dma((NZ,)),
            dma((NZ, 2)), dma((RT,)),
        ],
        compiler_params=pltpu.CompilerParams(
            has_side_effects=True, vmem_limit_bytes=48 * 1024 * 1024
        ),
    )(tile_values[0, 0], lists, dense_factor)


def solution(mesh):
    in_specs = (
        P("row", "col", None, None, None),
        P("row", "col", None),
        P("row", "col", None),
        P("row", "col", None),
        P("row", "col"),
    )
    out_specs = P("col", "row")
    return jax.shard_map(body, mesh=mesh, in_specs=in_specs, out_specs=out_specs, check_vma=False)
```

```python
import jax
import jax.numpy as jnp
from jax import lax
from jax.experimental import pallas as pl
from jax.experimental.pallas import tpu as pltpu
from jax.sharding import PartitionSpec as P

NX, NY, NZ = 4, 4, 8
TS = 128
SHARE = 32
RT = 16
CT = 64
SLOTS = 16
PER = 2
CHUNKS = SLOTS // PER
HALF = CHUNKS // 2
PIECES = 4
SPAN = CT * TS // (2 * PIECES)
MESH = pl.DeviceIdType.MESH


def rem(a, b):
    return lax.rem(a, jnp.int32(b))


def div(a, b):
    return lax.div(a, jnp.int32(b))


def kernel(
    tiles, rows_in, cols_in, live_in, dense, out,
    held, lists, lists_s, relay, both, split, acc, near, far, pair, done,
    local_sem, tile_sem, dense_sem,
    right_send, right_recv, left_send, left_recv, list_send, list_recv,
    hop1_send, hop1_recv, hop2_send, hop2_recv,
    near_send, near_recv, far_send, far_recv, pair_send, pair_recv, out_send, out_recv,
):
    row, col = lax.axis_index("row"), lax.axis_index("col")
    x_hi, z = div(row, NZ), rem(row, NZ)
    y, x_lo, core = div(col, 4), rem(div(col, 2), 2), rem(col, 2)
    x = x_hi * 2 + x_lo

    def device(x, y, z, core):
        return (div(x, 2) * NZ + z, y * 4 + rem(x, 2) * 2 + core)

    def copy(src, dst, send_sem, recv_sem, target):
        return pltpu.make_async_remote_copy(
            src_ref=src, dst_ref=dst, send_sem=send_sem, recv_sem=recv_sem,
            device_id=target, device_id_type=MESH,
        )

    up = device(x, y, rem(z + 1, NZ), core)
    down = device(x, y, rem(z + NZ - 1, NZ), core)
    forth = device(rem(x + 1, NX), y, z, core)
    back = device(rem(x + NX - 1, NX), y, z, core)

    barrier = pltpu.get_barrier_semaphore()
    partners = [up, down, forth, back, device(x, y, z, 1 - core)]
    partners += [device(x, rem(y + step, NY), z, core) for step in (1, 2, 3)]
    for partner in partners:
        pl.semaphore_signal(barrier, inc=1, device_id=partner, device_id_type=MESH)

    center = col - x_hi * NZ

    def banded(source):
        gap = source - center
        return jnp.logical_and(gap >= -1, gap <= 1)

    def right_hops(source, j):
        u = rem(source - center + 3 + 4 * NZ, NZ) - 3
        second = j >= HALF
        first_hops = jnp.where(u > 0, 4, 3)
        second_hops = jnp.where(u < 0, 2, jnp.where(u > 0, 5, 4))
        even_hops = jnp.where(rem(j, HALF) < HALF // 2, 4, 3)
        crossed = jnp.logical_and(center >= -1, center <= NZ)
        return jnp.where(crossed, jnp.where(second, second_hops, first_hops), even_hops)

    def ring_message(level, source, j, rightwards):
        there = jnp.logical_or(j < HALF, banded(source))
        hops = right_hops(source, j)
        if not rightwards:
            hops = NZ - 1 - hops
        there = jnp.logical_and(there, level < hops)
        part = held.at[source, pl.ds(PER * j, PER)]
        if rightwards:
            return there, copy(part, part, right_send.at[level, j], right_recv.at[level, j], up)
        return there, copy(part, part, left_send.at[level, j], left_recv.at[level, j], down)

    def around(distance, rightwards):
        return rem(z + NZ - distance, NZ) if rightwards else rem(z + distance, NZ)

    def ring_start(level, j):
        for way in (True, False):
            there, made = ring_message(level, around(level, way), j, way)
            pl.when(there)(made.start)

    def ring_wait(level, j):
        for way in (True, False):
            there, made = ring_message(level, around(level + 1, way), j, way)
            pl.when(there)(made.wait_recv)

    def ring_sent(level, j):
        for way in (True, False):
            there, made = ring_message(level, around(level, way), j, way)
            pl.when(there)(made.wait_send)

    def list_message(level, distance, rightwards):
        part = lists.at[around(distance, rightwards)]
        way = 0 if rightwards else 1
        return copy(
            part, part, list_send.at[way, level], list_recv.at[way, level],
            up if rightwards else down,
        )

    def list_start(level):
        for way in (True, False)[: 2 if level < 3 else 1]:
            list_message(level, level, way).start()

    def list_wait(level):
        for way in (True, False)[: 2 if level < 3 else 1]:
            list_message(level, level + 1, way).wait_recv()

    def columns(way, k):
        return pl.ds(pl.multiple_of((way * PIECES + k) * SPAN, SPAN), SPAN)

    def hop1(way, k):
        return copy(
            both.at[x_hi, :, columns(way, k)], relay.at[way, k],
            hop1_send.at[way, k], hop1_recv.at[way, k], (forth, back)[way],
        )

    def hop2(way, k, owner):
        return copy(
            relay.at[way, k], both.at[owner, :, columns(way, k)],
            hop2_send.at[way, k], hop2_recv.at[way, k], (forth, back)[way],
        )

    def relayed(way):
        return div(rem(x + (NX - 1 if way == 0 else 1), NX), 2)

    own_lists = [
        pltpu.make_async_copy(ref, lists.at[z, k], local_sem.at[k])
        for k, ref in enumerate((rows_in, cols_in, live_in))
    ]

    def own_tiles(j):
        part = pl.ds(PER * j, PER)
        return pltpu.make_async_copy(tiles.at[part], held.at[z, part], tile_sem.at[j])

    def own_dense(way, k):
        part = columns(way, k)
        return pltpu.make_async_copy(
            dense.at[:, part], both.at[x_hi, :, part], dense_sem.at[way, k]
        )

    for made in own_lists:
        made.start()

    @pl.loop(0, CHUNKS)
    def _(j):
        own_tiles(j).start()

    @pl.loop(0, PIECES)
    def _(k):
        for way in (0, 1):
            own_dense(way, k).start()

    for made in own_lists:
        made.wait()
    pl.semaphore_wait(barrier, len(partners))
    list_start(0)

    @pl.loop(0, CHUNKS)
    def _(j):
        own_tiles(j).wait()
        ring_start(0, j)

        @pl.when(j < PIECES)
        def _():
            for way in (0, 1):
                own_dense(way, j).wait()
                hop1(way, j).start()

    @pl.loop(0, NZ * RT)
    def _(i):
        acc[div(i, RT), rem(i, RT)] = jnp.zeros((2 * SHARE, TS), jnp.float32)

    def one_tile(b, slot):
        tile = held[b, slot]
        high = tile.astype(jnp.bfloat16)
        low = (tile - high.astype(jnp.float32)).astype(jnp.bfloat16)
        chosen = split[lists_s[b, 1, 0, slot]]
        dims = (((1,), (1,)), ((), ()))
        by_high = lax.dot_general(chosen, high, dims, preferred_element_type=jnp.float32)
        by_low = lax.dot_general(
            chosen[: 2 * SHARE], low, dims, preferred_element_type=jnp.float32
        )
        return by_high[: 2 * SHARE] + (by_high[2 * SHARE :] + by_low)

    def multiply(b, j):
        @pl.when(jnp.logical_or(j < HALF, banded(b)))
        def _():
            products = [one_tile(b, PER * j + s) for s in range(PER)]
            for k in range(RT):
                term = acc[b, k]
                for s in range(PER):
                    slot = PER * j + s
                    live = lists_s[b, 2, 0, slot].astype(jnp.float32)
                    weight = jnp.where(lists_s[b, 0, 0, slot] == k, live, 0.0)
                    term = term + weight * products[s]
                acc[b, k] = term

    def near_copy(b):
        return copy(
            acc.at[b, pl.ds((1 - core) * 8, 8)], near.at[b],
            near_send.at[b], near_recv.at[b], device(x, y, z, 1 - core),
        )

    def far_copy(b, step):
        there = rem(y + step, NY)
        return copy(
            acc.at[b, pl.ds(core * 8 + there * 2, 2)], far.at[b, step - 1],
            far_send.at[b, step - 1], far_recv.at[b, step - 1], device(x, there, z, core),
        )

    def pair_copy(b):
        return copy(
            acc.at[b, core * 8 + y * 2 + (1 - x_lo)], pair.at[b],
            pair_send.at[b], pair_recv.at[b], device(x_hi * 2 + 1 - x_lo, y, z, core),
        )

    mine = core * 8 + y * 2 + x_lo

    def out_copy(b, a):
        return copy(
            done.at[b, pl.ds(a * SHARE, SHARE)], out.at[:, pl.ds(pl.multiple_of(mine * TS, TS), TS)],
            out_send.at[b, a], out_recv.at[mine], (x_hi * NZ + b, a * NZ + z),
        )

    def block(i):
        return rem(z + i + NZ, NZ)

    def stage1(i):
        near_copy(block(i)).start()

    def stage2(i):
        b = block(i)
        near_copy(b).wait_recv()

        @pl.loop(0, 8)
        def _(k):
            acc[b, core * 8 + k] = acc[b, core * 8 + k] + near[b, k]

        for step in (1, 2, 3):
            far_copy(b, step).start()

    def stage3(i):
        b = block(i)
        for step in (1, 2, 3):
            far_copy(b, step).wait_recv()
        for k in range(2):
            place = core * 8 + y * 2 + k
            acc[b, place] = acc[b, place] + (far[b, 0, k] + far[b, 1, k] + far[b, 2, k])
        pair_copy(b).start()

    def is_home(b, a):
        return jnp.logical_and(b == z, a * NZ + z == col)

    def stage4(i):
        b = block(i)
        pair_copy(b).wait_recv()
        done[b] = acc[b, mine] + pair[b]
        for a in range(2):
            home = is_home(b, a)

            @pl.when(home)
            def _():
                out[:, pl.ds(pl.multiple_of(mine * TS, TS), TS)] = done[b, a * SHARE : (a + 1) * SHARE]

            @pl.when(jnp.logical_not(home))
            def _():
                out_copy(b, a).start()

    @pl.loop(0, CHUNKS)
    def _(j):
        @pl.when(j < PIECES)
        def _():
            for way in (0, 1):
                hop1(way, j).wait_recv()
                hop2(way, j, relayed(way)).start()

        ring_wait(0, j)
        ring_start(1, j)
        for level in range(4):
            @pl.when(j == level)
            def _():
                list_wait(level)
                if level < 3:
                    list_start(level + 1)

    @pl.loop(0, HALF)
    def _(j):
        ring_wait(1, j)
        ring_start(2, j)

    to_scalar = pltpu.make_async_copy(lists, lists_s, local_sem.at[0])
    to_scalar.start()

    @pl.loop(0, PIECES)
    def _(k):
        for way in (0, 1):
            hop2(way, k, 1 - x_hi).wait_recv()

    @pl.loop(0, CT)
    def _(t):
        place = pl.ds(pl.multiple_of(t * TS, TS), TS)
        for a in range(2):
            value = both[a, :, place]
            high = value.astype(jnp.bfloat16)
            low = (value - high.astype(jnp.float32)).astype(jnp.bfloat16)
            split[t, a * SHARE : (a + 1) * SHARE] = high
            split[t, (2 + a) * SHARE : (3 + a) * SHARE] = low

    to_scalar.wait()

    @pl.loop(HALF, CHUNKS)
    def _(j):
        ring_wait(1, j)
        ring_start(2, j)

        @pl.loop(0, 3)
        def _(i):
            multiply(block(i - 1), j - HALF)
            multiply(block(i - 1), j)

    stage1(0)
    stage1(1)
    stage1(-1)

    @pl.loop(0, CHUNKS)
    def _(j):
        ring_wait(2, j)
        ring_start(3, j)
        multiply(block(2), j)
        multiply(block(-2), j)
        for i, when in ((0, 0), (1, 1), (-1, 2)):
            pl.when(j == when)(lambda i=i: stage2(i))

    stage1(2)
    stage1(-2)

    @pl.loop(0, CHUNKS)
    def _(j):
        ring_wait(3, j)
        ring_start(4, j)
        multiply(block(4), j)

        @pl.when(j < HALF)
        def _():
            multiply(block(3), j)
            multiply(block(-3), j)

        for i, when in ((2, 0), (-2, 1)):
            pl.when(j == when)(lambda i=i: stage2(i))
        for i, when in ((0, 2), (1, 3), (-1, 3)):
            pl.when(j == when)(lambda i=i: stage3(i))

    stage1(4)

    @pl.loop(HALF, CHUNKS)
    def _(j):
        ring_wait(4, j)
        multiply(block(3), j)
        multiply(block(-3), j)

    stage1(3)
    stage1(-3)
    for i in (0, 1, -1):
        stage4(i)
    stage2(4)
    stage3(2)
    stage3(-2)
    stage2(3)
    stage2(-3)
    stage4(2)
    stage4(-2)
    stage3(4)
    stage3(3)
    stage3(-3)
    stage4(4)
    stage4(3)
    stage4(-3)

    @pl.loop(0, RT)
    def _(t):
        source = (div(rem(t, 8), 2) * 2 + rem(t, 2)) * 2 + div(t, 8)
        there = out.at[:, pl.ds(pl.multiple_of(t * TS, TS), TS)]
        home = jnp.logical_and(source == col, rem(col, NZ) == z)

        @pl.when(jnp.logical_not(home))
        def _():
            copy(
                done.at[0, pl.ds(0, SHARE)], there, out_send.at[0, 0], out_recv.at[t],
                (row, rem(col + 1, 16)),
            ).wait_recv()

    for level in range(4):
        for way in (True, False)[: 2 if level < 3 else 1]:
            list_message(level, level, way).wait_send()

    @pl.loop(0, CHUNKS)
    def _(j):
        for level in range(5):
            ring_sent(level, j)

    @pl.loop(0, PIECES)
    def _(k):
        for way in (0, 1):
            hop1(way, k).wait_send()
            hop2(way, k, relayed(way)).wait_send()

    @pl.loop(0, NZ)
    def _(b):
        near_copy(b).wait_send()
        for step in (1, 2, 3):
            far_copy(b, step).wait_send()
        pair_copy(b).wait_send()
        for a in range(2):
            pl.when(jnp.logical_not(is_home(b, a)))(out_copy(b, a).wait_send)


def body(tile_values, tile_rows, tile_cols, tile_live, dense_factor):
    dma = pltpu.SemaphoreType.DMA
    vmem = pltpu.VMEM
    f32 = jnp.float32
    return pl.pallas_call(
        kernel,
        out_shape=jax.ShapeDtypeStruct((SHARE, RT * TS), f32),
        in_specs=[pl.BlockSpec(memory_space=pltpu.HBM)] * 5,
        out_specs=pl.BlockSpec(memory_space=pltpu.VMEM),
        scratch_shapes=[
            vmem((NZ, SLOTS, TS, TS), f32),
            vmem((NZ, 3, 1, SLOTS), jnp.int32),
            pltpu.SMEM((NZ, 3, 1, SLOTS), jnp.int32),
            vmem((2, PIECES, SHARE, SPAN), f32),
            vmem((2, SHARE, CT * TS), f32),
            vmem((CT, 4 * SHARE, TS), jnp.bfloat16),
            vmem((NZ, RT, 2 * SHARE, TS), f32),
            vmem((NZ, 8, 2 * SHARE, TS), f32),
            vmem((NZ, 3, 2, 2 * SHARE, TS), f32),
            vmem((NZ, 2 * SHARE, TS), f32),
            vmem((NZ, 2 * SHARE, TS), f32),
            dma((3,)), dma((CHUNKS,)), dma((2, PIECES)),
            dma((5, CHUNKS)), dma((5, CHUNKS)), dma((5, CHUNKS)), dma((5, CHUNKS)),
            dma((2, 4)), dma((2, 4)),
            dma((2, PIECES)), dma((2, PIECES)), dma((2, PIECES)), dma((2, PIECES)),
            dma((NZ,)), dma((NZ,)), dma((NZ, 3)), dma((NZ, 3)), dma((NZ,)), dma((NZ,)),
            dma((NZ, 2)), dma((RT,)),
        ],
        compiler_params=pltpu.CompilerParams(
            collective_id=0, has_side_effects=True, vmem_limit_bytes=48 * 1024 * 1024
        ),
    )(tile_values[0, 0], tile_rows[0], tile_cols[0], tile_live[0], dense_factor)


def solution(mesh):
    in_specs = (
        P("row", "col", None, None, None),
        P("row", "col", None),
        P("row", "col", None),
        P("row", "col", None),
        P("row", "col"),
    )
    out_specs = P("col", "row")
    return jax.shard_map(body, mesh=mesh, in_specs=in_specs, out_specs=out_specs, check_vma=False)
```

```python
import jax
import jax.numpy as jnp
from jax import lax
from jax.experimental import pallas as pl
from jax.experimental.pallas import tpu as pltpu
from jax.sharding import PartitionSpec as P

NX, NY, NZ = 4, 4, 8
TS = 128
SHARE = 32
RT = 16
CT = 64
SLOTS = 16
PER = 2
CHUNKS = SLOTS // PER
HALF = CHUNKS // 2
PIECES = 4
SPAN = CT * TS // (2 * PIECES)
MESH = pl.DeviceIdType.MESH


def rem(a, b):
    return lax.rem(a, jnp.int32(b))


def div(a, b):
    return lax.div(a, jnp.int32(b))


def kernel(
    tiles, rows_in, cols_in, live_in, dense, out,
    held, lists, lists_s, relay, both, split, acc, near, far, pair, done,
    local_sem, tile_sem, dense_sem,
    right_send, right_recv, left_send, left_recv, list_send, list_recv,
    hop1_send, hop1_recv, hop2_send, hop2_recv,
    near_send, near_recv, far_send, far_recv, pair_send, pair_recv, out_send, out_recv,
):
    row, col = lax.axis_index("row"), lax.axis_index("col")
    x_hi, z = div(row, NZ), rem(row, NZ)
    y, x_lo, core = div(col, 4), rem(div(col, 2), 2), rem(col, 2)
    x = x_hi * 2 + x_lo

    def device(x, y, z, core):
        return (div(x, 2) * NZ + z, y * 4 + rem(x, 2) * 2 + core)

    def copy(src, dst, send_sem, recv_sem, target):
        return pltpu.make_async_remote_copy(
            src_ref=src, dst_ref=dst, send_sem=send_sem, recv_sem=recv_sem,
            device_id=target, device_id_type=MESH,
        )

    up = device(x, y, rem(z + 1, NZ), core)
    down = device(x, y, rem(z + NZ - 1, NZ), core)
    forth = device(rem(x + 1, NX), y, z, core)
    back = device(rem(x + NX - 1, NX), y, z, core)

    barrier = pltpu.get_barrier_semaphore()
    partners = [device(x, y, rem(z + step, NZ), core) for step in range(1, NZ)]
    partners += [forth, back, device(x, y, z, 1 - core)]
    partners += [device(x, rem(y + step, NY), z, core) for step in (1, 2, 3)]
    for partner in partners:
        pl.semaphore_signal(barrier, inc=1, device_id=partner, device_id_type=MESH)

    center = col - x_hi * NZ

    def banded(source):
        gap = source - center
        return jnp.logical_and(gap >= -1, gap <= 1)

    def right_hops(source, j):
        u = rem(source - center + 3 + 4 * NZ, NZ) - 3
        second = j >= HALF
        first_hops = jnp.where(u > 0, 4, 3)
        second_hops = jnp.where(u < 0, 2, jnp.where(u > 0, 5, 4))
        even_hops = jnp.where(rem(j, HALF) < HALF // 2, 4, 3)
        crossed = jnp.logical_and(center >= -1, center <= NZ)
        return jnp.where(crossed, jnp.where(second, second_hops, first_hops), even_hops)

    def ring_message(level, source, j, rightwards):
        there = jnp.logical_or(j < HALF, banded(source))
        hops = right_hops(source, j)
        if not rightwards:
            hops = NZ - 1 - hops
        there = jnp.logical_and(there, level < hops)
        part = held.at[source, pl.ds(PER * j, PER)]
        if rightwards:
            return there, copy(part, part, right_send.at[level, j], right_recv.at[level, j], up)
        return there, copy(part, part, left_send.at[level, j], left_recv.at[level, j], down)

    def around(distance, rightwards):
        return rem(z + NZ - distance, NZ) if rightwards else rem(z + distance, NZ)

    def ring_start(level, j):
        for way in (True, False):
            there, made = ring_message(level, around(level, way), j, way)
            pl.when(there)(made.start)

    def ring_wait(level, j):
        for way in (True, False):
            there, made = ring_message(level, around(level + 1, way), j, way)
            pl.when(there)(made.wait_recv)

    def ring_sent(level, j):
        for way in (True, False):
            there, made = ring_message(level, around(level, way), j, way)
            pl.when(there)(made.wait_send)

    def list_copy(p):
        peer = rem(z + p, NZ)
        return copy(
            lists.at[z], lists.at[z], list_send.at[p], list_recv.at[z], device(x, y, peer, core)
        )

    def list_arrival(p):
        peer = rem(z + p, NZ)
        return copy(
            lists.at[peer], lists.at[peer], list_send.at[p], list_recv.at[peer],
            device(x, y, peer, core),
        )

    def columns(way, k):
        return pl.ds(pl.multiple_of((way * PIECES + k) * SPAN, SPAN), SPAN)

    def hop1(way, k):
        return copy(
            both.at[x_hi, :, columns(way, k)], relay.at[way, k],
            hop1_send.at[way, k], hop1_recv.at[way, k], (forth, back)[way],
        )

    def hop2(way, k, owner):
        return copy(
            relay.at[way, k], both.at[owner, :, columns(way, k)],
            hop2_send.at[way, k], hop2_recv.at[way, k], (forth, back)[way],
        )

    def relayed(way):
        return div(rem(x + (NX - 1 if way == 0 else 1), NX), 2)

    own_lists = [
        pltpu.make_async_copy(ref, lists.at[z, k], local_sem.at[k])
        for k, ref in enumerate((rows_in, cols_in, live_in))
    ]

    def own_tiles(j):
        part = pl.ds(PER * j, PER)
        return pltpu.make_async_copy(tiles.at[part], held.at[z, part], tile_sem.at[j])

    def own_dense(way, k):
        part = columns(way, k)
        return pltpu.make_async_copy(
            dense.at[:, part], both.at[x_hi, :, part], dense_sem.at[way, k]
        )

    for made in own_lists:
        made.start()

    @pl.loop(0, CHUNKS)
    def _(j):
        own_tiles(j).start()

    @pl.loop(0, PIECES)
    def _(k):
        for way in (0, 1):
            own_dense(way, k).start()

    for made in own_lists:
        made.wait()
    pl.semaphore_wait(barrier, len(partners))

    @pl.loop(1, NZ)
    def _(p):
        list_copy(p).start()

    @pl.loop(0, CHUNKS)
    def _(j):
        own_tiles(j).wait()
        ring_start(0, j)

        @pl.when(j < PIECES)
        def _():
            for way in (0, 1):
                own_dense(way, j).wait()
                hop1(way, j).start()

    @pl.loop(0, NZ * RT)
    def _(i):
        acc[div(i, RT), rem(i, RT)] = jnp.zeros((2 * SHARE, TS), jnp.float32)

    def one_tile(b, slot):
        tile = held[b, slot]
        high = tile.astype(jnp.bfloat16)
        low = (tile - high.astype(jnp.float32)).astype(jnp.bfloat16)
        chosen = split[lists_s[b, 1, 0, slot]]
        dims = (((1,), (1,)), ((), ()))
        by_high = lax.dot_general(chosen, high, dims, preferred_element_type=jnp.float32)
        by_low = lax.dot_general(
            chosen[: 2 * SHARE], low, dims, preferred_element_type=jnp.float32
        )
        return by_high[: 2 * SHARE] + (by_high[2 * SHARE :] + by_low)

    def multiply(b, j):
        @pl.when(jnp.logical_or(j < HALF, banded(b)))
        def _():
            products = [one_tile(b, PER * j + s) for s in range(PER)]
            for k in range(RT):
                term = acc[b, k]
                for s in range(PER):
                    slot = PER * j + s
                    live = lists_s[b, 2, 0, slot].astype(jnp.float32)
                    weight = jnp.where(lists_s[b, 0, 0, slot] == k, live, 0.0)
                    term = term + weight * products[s]
                acc[b, k] = term

    def near_copy(b):
        return copy(
            acc.at[b, pl.ds((1 - core) * 8, 8)], near.at[b],
            near_send.at[b], near_recv.at[b], device(x, y, z, 1 - core),
        )

    def far_copy(b, step):
        there = rem(y + step, NY)
        return copy(
            acc.at[b, pl.ds(core * 8 + there * 2, 2)], far.at[b, step - 1],
            far_send.at[b, step - 1], far_recv.at[b, step - 1], device(x, there, z, core),
        )

    def pair_copy(b):
        return copy(
            acc.at[b, core * 8 + y * 2 + (1 - x_lo)], pair.at[b],
            pair_send.at[b], pair_recv.at[b], device(x_hi * 2 + 1 - x_lo, y, z, core),
        )

    mine = core * 8 + y * 2 + x_lo

    def out_copy(b, a):
        return copy(
            done.at[b, pl.ds(a * SHARE, SHARE)], out.at[:, pl.ds(pl.multiple_of(mine * TS, TS), TS)],
            out_send.at[b, a], out_recv.at[mine], (x_hi * NZ + b, a * NZ + z),
        )

    def block(i):
        return rem(z + i + NZ, NZ)

    def stage1(i):
        near_copy(block(i)).start()

    def stage2(i):
        b = block(i)
        near_copy(b).wait_recv()

        @pl.loop(0, 8)
        def _(k):
            acc[b, core * 8 + k] = acc[b, core * 8 + k] + near[b, k]

        for step in (1, 2, 3):
            far_copy(b, step).start()

    def stage3(i):
        b = block(i)
        for step in (1, 2, 3):
            far_copy(b, step).wait_recv()
        for k in range(2):
            place = core * 8 + y * 2 + k
            acc[b, place] = acc[b, place] + (far[b, 0, k] + far[b, 1, k] + far[b, 2, k])
        pair_copy(b).start()

    def is_home(b, a):
        return jnp.logical_and(b == z, a * NZ + z == col)

    def stage4(i):
        b = block(i)
        pair_copy(b).wait_recv()
        done[b] = acc[b, mine] + pair[b]
        for a in range(2):
            home = is_home(b, a)

            @pl.when(home)
            def _():
                out[:, pl.ds(pl.multiple_of(mine * TS, TS), TS)] = done[b, a * SHARE : (a + 1) * SHARE]

            @pl.when(jnp.logical_not(home))
            def _():
                out_copy(b, a).start()

    @pl.loop(0, CHUNKS)
    def _(j):
        @pl.when(j < PIECES)
        def _():
            for way in (0, 1):
                hop1(way, j).wait_recv()
                hop2(way, j, relayed(way)).start()

        ring_wait(0, j)
        ring_start(1, j)

    @pl.loop(0, HALF)
    def _(j):
        ring_wait(1, j)
        ring_start(2, j)

    @pl.loop(1, NZ)
    def _(p):
        list_arrival(p).wait_recv()

    to_scalar = pltpu.make_async_copy(lists, lists_s, local_sem.at[0])
    to_scalar.start()

    @pl.loop(0, PIECES)
    def _(k):
        for way in (0, 1):
            hop2(way, k, 1 - x_hi).wait_recv()

    @pl.loop(0, CT)
    def _(t):
        place = pl.ds(pl.multiple_of(t * TS, TS), TS)
        for a in range(2):
            value = both[a, :, place]
            high = value.astype(jnp.bfloat16)
            low = (value - high.astype(jnp.float32)).astype(jnp.bfloat16)
            split[t, a * SHARE : (a + 1) * SHARE] = high
            split[t, (2 + a) * SHARE : (3 + a) * SHARE] = low

    to_scalar.wait()

    @pl.loop(HALF, CHUNKS)
    def _(j):
        ring_wait(1, j)
        ring_start(2, j)

        @pl.loop(0, 3)
        def _(i):
            multiply(block(i - 1), j - HALF)
            multiply(block(i - 1), j)

    stage1(0)
    stage1(1)
    stage1(-1)

    @pl.loop(0, CHUNKS)
    def _(j):
        ring_wait(2, j)
        ring_start(3, j)
        multiply(block(2), j)
        multiply(block(-2), j)
        for i, when in ((0, 0), (1, 1), (-1, 2)):
            pl.when(j == when)(lambda i=i: stage2(i))

    stage1(2)
    stage1(-2)

    @pl.loop(0, CHUNKS)
    def _(j):
        ring_wait(3, j)
        ring_start(4, j)
        multiply(block(4), j)

        @pl.when(j < HALF)
        def _():
            multiply(block(3), j)
            multiply(block(-3), j)

        for i, when in ((2, 0), (-2, 1)):
            pl.when(j == when)(lambda i=i: stage2(i))
        for i, when in ((0, 2), (1, 3), (-1, 3)):
            pl.when(j == when)(lambda i=i: stage3(i))

    stage1(4)

    @pl.loop(HALF, CHUNKS)
    def _(j):
        ring_wait(4, j)
        multiply(block(3), j)
        multiply(block(-3), j)

    stage1(3)
    stage1(-3)
    for i in (0, 1, -1):
        stage4(i)
    stage2(4)
    stage3(2)
    stage3(-2)
    stage2(3)
    stage2(-3)
    stage4(2)
    stage4(-2)
    stage3(4)
    stage3(3)
    stage3(-3)
    stage4(4)
    stage4(3)
    stage4(-3)

    @pl.loop(0, RT)
    def _(t):
        source = (div(rem(t, 8), 2) * 2 + rem(t, 2)) * 2 + div(t, 8)
        there = out.at[:, pl.ds(pl.multiple_of(t * TS, TS), TS)]
        home = jnp.logical_and(source == col, rem(col, NZ) == z)

        @pl.when(jnp.logical_not(home))
        def _():
            copy(
                done.at[0, pl.ds(0, SHARE)], there, out_send.at[0, 0], out_recv.at[t],
                (row, rem(col + 1, 16)),
            ).wait_recv()

    @pl.loop(1, NZ)
    def _(p):
        list_copy(p).wait_send()

    @pl.loop(0, CHUNKS)
    def _(j):
        for level in range(5):
            ring_sent(level, j)

    @pl.loop(0, PIECES)
    def _(k):
        for way in (0, 1):
            hop1(way, k).wait_send()
            hop2(way, k, relayed(way)).wait_send()

    @pl.loop(0, NZ)
    def _(b):
        near_copy(b).wait_send()
        for step in (1, 2, 3):
            far_copy(b, step).wait_send()
        pair_copy(b).wait_send()
        for a in range(2):
            pl.when(jnp.logical_not(is_home(b, a)))(out_copy(b, a).wait_send)


def body(tile_values, tile_rows, tile_cols, tile_live, dense_factor):
    dma = pltpu.SemaphoreType.DMA
    vmem = pltpu.VMEM
    f32 = jnp.float32
    return pl.pallas_call(
        kernel,
        out_shape=jax.ShapeDtypeStruct((SHARE, RT * TS), f32),
        in_specs=[pl.BlockSpec(memory_space=pltpu.HBM)] * 5,
        out_specs=pl.BlockSpec(memory_space=pltpu.VMEM),
        scratch_shapes=[
            vmem((NZ, SLOTS, TS, TS), f32),
            vmem((NZ, 3, 1, SLOTS), jnp.int32),
            pltpu.SMEM((NZ, 3, 1, SLOTS), jnp.int32),
            vmem((2, PIECES, SHARE, SPAN), f32),
            vmem((2, SHARE, CT * TS), f32),
            vmem((CT, 4 * SHARE, TS), jnp.bfloat16),
            vmem((NZ, RT, 2 * SHARE, TS), f32),
            vmem((NZ, 8, 2 * SHARE, TS), f32),
            vmem((NZ, 3, 2, 2 * SHARE, TS), f32),
            vmem((NZ, 2 * SHARE, TS), f32),
            vmem((NZ, 2 * SHARE, TS), f32),
            dma((3,)), dma((CHUNKS,)), dma((2, PIECES)),
            dma((5, CHUNKS)), dma((5, CHUNKS)), dma((5, CHUNKS)), dma((5, CHUNKS)),
            dma((NZ,)), dma((NZ,)),
            dma((2, PIECES)), dma((2, PIECES)), dma((2, PIECES)), dma((2, PIECES)),
            dma((NZ,)), dma((NZ,)), dma((NZ, 3)), dma((NZ, 3)), dma((NZ,)), dma((NZ,)),
            dma((NZ, 2)), dma((RT,)),
        ],
        compiler_params=pltpu.CompilerParams(
            collective_id=0, has_side_effects=True, vmem_limit_bytes=67043328
        ),
    )(tile_values[0, 0], tile_rows[0], tile_cols[0], tile_live[0], dense_factor)


def solution(mesh):
    in_specs = (
        P("row", "col", None, None, None),
        P("row", "col", None),
        P("row", "col", None),
        P("row", "col", None),
        P("row", "col"),
    )
    out_specs = P("col", "row")
    return jax.shard_map(body, mesh=mesh, in_specs=in_specs, out_specs=out_specs, check_vma=False)
```

```python
import jax
import jax.numpy as jnp
from jax import lax
from jax.experimental import pallas as pl
from jax.experimental.pallas import tpu as pltpu
from jax.sharding import PartitionSpec as P

NX, NY, NZ = 4, 4, 8
TS = 128
SHARE = 32
RT = 16
CT = 64
SLOTS = 16
PER = 2
CHUNKS = SLOTS // PER
HALF = CHUNKS // 2
PIECES = 4
SPAN = CT * TS // (2 * PIECES)
GROUPS = 5
TICKS = GROUPS * HALF
NONE = 2 * GROUPS
FIRST = 7
MOST = 4
PLAN = (
    (2, 0, 9), (2, 1, 10), (2, -1, 11), (3, 0, 12), (3, 1, 13), (3, -1, 14),
    (4, 0, 15), (4, 1, 16), (4, -1, 16), (2, 2, 17), (2, -2, 17),
)
REST = (
    (3, 2), (3, -2), (2, 4), (2, 3), (2, -3), (4, 2), (4, -2),
    (3, 4), (3, 3), (3, -3), (4, 4), (4, 3), (4, -3),
)
MESH = pl.DeviceIdType.MESH


def rem(a, b):
    return lax.rem(a, jnp.int32(b))


def div(a, b):
    return lax.div(a, jnp.int32(b))


def kernel(
    tiles, rows_in, cols_in, live_in, dense, out,
    held, lists, lists_s, relay, both, split, acc, near, far, pair, done,
    local_sem,
    right_send, right_recv, left_send, left_recv, list_send, list_recv,
    hop1_send, hop1_recv, hop2_send, hop2_recv,
    near_send, near_recv, far_send, far_recv, pair_send, pair_recv, out_send, out_recv,
):
    row, col = lax.axis_index("row"), lax.axis_index("col")
    x_hi, z = div(row, NZ), rem(row, NZ)
    y, x_lo, core = div(col, 4), rem(div(col, 2), 2), rem(col, 2)
    x = x_hi * 2 + x_lo

    def device(x, y, z, core):
        return (div(x, 2) * NZ + z, y * 4 + rem(x, 2) * 2 + core)

    def copy(src, dst, send_sem, recv_sem, target):
        return pltpu.make_async_remote_copy(
            src_ref=src, dst_ref=dst, send_sem=send_sem, recv_sem=recv_sem,
            device_id=target, device_id_type=MESH,
        )

    up = device(x, y, rem(z + 1, NZ), core)
    down = device(x, y, rem(z + NZ - 1, NZ), core)
    forth = device(rem(x + 1, NX), y, z, core)
    back = device(rem(x + NX - 1, NX), y, z, core)

    barrier = pltpu.get_barrier_semaphore()
    partners = [device(x, y, rem(z + step, NZ), core) for step in range(1, NZ)]
    partners += [forth, back, device(x, y, z, 1 - core)]
    partners += [device(x, rem(y + step, NY), z, core) for step in (1, 2, 3)]
    for partner in partners:
        pl.semaphore_signal(barrier, inc=1, device_id=partner, device_id_type=MESH)

    center = col - x_hi * NZ

    def banded(source):
        gap = source - center
        return jnp.logical_and(gap >= -1, gap <= 1)

    crossed = jnp.logical_and(center >= -1, center <= NZ)

    def place(source):
        return rem(source - center + 3 + 4 * NZ, NZ) - 3

    def hops(source, half, way):
        u = place(source)
        first = jnp.where(u > 0, 4, 3)
        second = jnp.where(u < 0, 2, jnp.where(u > 0, 5, 4))
        even = 3 + rem(source, 2)
        rightwards = jnp.where(crossed, jnp.where(half == 1, second, first), even)
        return rightwards if way == 0 else NZ - 1 - rightwards

    def half_of(source, turn, way):
        swap = (place(source) >= 0) if way == 0 else (place(source) < 0)
        return rem(turn + jnp.where(swap, 1, 0), 2)

    def travels(source, half, level, way):
        there = jnp.logical_or(half == 0, banded(source))
        return jnp.logical_and(there, level < hops(source, half, way))

    def source_of(level, way):
        return rem(z + 2 * NZ + (-level - 1 if way == 0 else level + 1), NZ)

    own_groups = jnp.where(banded(z), 2, 1)
    coming, passed, onward = [], [], []
    for way in (0, 1):
        group = [jnp.int32(NONE)] * GROUPS
        count = jnp.int32(0)
        for g in range(2 * GROUPS):
            source = source_of(g // 2, way)
            there = travels(source, half_of(source, g % 2, way), g // 2, way)
            for n in range(GROUPS):
                group[n] = jnp.where(jnp.logical_and(there, count == n), g, group[n])
            count = count + jnp.where(there, 1, 0)
        coming.append(group)
        goes, slots = [], []
        slot = own_groups
        for n in range(GROUPS):
            level = div(group[n], 2)
            source = source_of(level, way)
            on = travels(source, half_of(source, rem(group[n], 2), way), level + 1, way)
            on = jnp.logical_and(on, group[n] < NONE)
            goes.append(jnp.where(on, 1, 0))
            slots.append(slot)
            slot = slot + goes[-1]
        passed.append(goes)
        onward.append(slots)

    def pick(values, n):
        chosen = values[0]
        for i in range(1, GROUPS):
            chosen = jnp.where(n == i, values[i], chosen)
        return chosen

    def ring_copy(source, j, slot, way):
        part = held.at[source, pl.ds(PER * j, PER)]
        if way == 0:
            return copy(part, part, right_send.at[slot], right_recv.at[slot], up)
        return copy(part, part, left_send.at[slot], left_recv.at[slot], down)

    def message(t, way):
        group = pick(coming[way], div(t, HALF))
        source = source_of(div(group, 2), way)
        j = half_of(source, rem(group, 2), way) * HALF + rem(t, HALF)
        return group < NONE, source, j

    def arrive(t, way):
        there, source, j = message(t, way)

        @pl.when(there)
        def _():
            ring_copy(source, j, t, way).wait_recv()
            n = div(t, HALF)

            @pl.when(pick(passed[way], n) == 1)
            def _():
                ring_copy(source, j, pick(onward[way], n) * HALF + rem(t, HALF), way).start()

    def own_message(k, way):
        turn = div(k, HALF)
        half = jnp.where(own_groups == 2, half_of(z, turn, way), 0)
        return turn < own_groups, ring_copy(z, half * HALF + rem(k, HALF), k, way)

    def ring_sent(k, way):
        made = ring_copy(z, 0, k, way)
        slot = div(k, HALF)
        count = own_groups
        for n in range(GROUPS):
            count = count + passed[way][n]
        pl.when(slot < count)(made.wait_send)

    def list_copy(p):
        peer = rem(z + p, NZ)
        return copy(lists.at[z], lists.at[z], list_send, list_recv, device(x, y, peer, core))

    seven = lists.at[pl.ds(0, NZ - 1)]
    all_lists = copy(seven, seven, list_send, list_recv, up)

    def columns(way, k):
        return pl.ds(pl.multiple_of((way * PIECES + k) * SPAN, SPAN), SPAN)

    def hop1(way, k):
        return copy(
            both.at[x_hi, :, columns(way, k)], relay.at[way, k],
            hop1_send.at[way], hop1_recv.at[way, k], (forth, back)[way],
        )

    def hop2(way, k, owner):
        return copy(
            relay.at[way, k], both.at[owner, :, columns(way, k)],
            hop2_send.at[way], hop2_recv.at[way], (forth, back)[way],
        )

    def all_pieces(way):
        part = both.at[1 - x_hi, :, pl.ds(way * PIECES * SPAN, PIECES * SPAN)]
        return (
            copy(part, part, hop1_send.at[way], hop2_recv.at[way], forth),
            copy(part, part, hop2_send.at[way], hop2_recv.at[way], forth),
        )

    def relayed(way):
        return div(rem(x + (NX - 1 if way == 0 else 1), NX), 2)

    own_lists = [
        pltpu.make_async_copy(ref, lists.at[z, k], local_sem.at[k])
        for k, ref in enumerate((rows_in, cols_in, live_in))
    ]

    own_tiles = pltpu.make_async_copy(tiles, held.at[z], local_sem.at[3])
    own_dense = pltpu.make_async_copy(dense, both.at[x_hi], local_sem.at[4])
    for made in own_lists:
        made.start()
    own_tiles.start()
    own_dense.start()

    for made in own_lists:
        made.wait()
    own_tiles.wait()
    pl.semaphore_wait(barrier, len(partners))

    @pl.loop(1, NZ)
    def _(p):
        list_copy(p).start()

    @pl.loop(0, CHUNKS)
    def _(k):
        for way in (0, 1):
            there, made = own_message(k, way)
            pl.when(there)(made.start)

    own_dense.wait()

    @pl.loop(0, PIECES)
    def _(k):
        for way in (0, 1):
            hop1(way, k).start()

    @pl.loop(0, NZ * RT)
    def _(i):
        acc[div(i, RT), rem(i, RT)] = jnp.zeros((2 * SHARE, TS), jnp.float32)

    def one_tile(b, slot):
        tile = held[b, slot]
        high = tile.astype(jnp.bfloat16)
        low = (tile - high.astype(jnp.float32)).astype(jnp.bfloat16)
        chosen = split[lists_s[b, 1, 0, slot]]
        dims = (((1,), (1,)), ((), ()))
        by_high = lax.dot_general(chosen, high, dims, preferred_element_type=jnp.float32)
        by_low = lax.dot_general(
            chosen[: 2 * SHARE], low, dims, preferred_element_type=jnp.float32
        )
        return by_high[: 2 * SHARE] + (by_high[2 * SHARE :] + by_low)

    def multiply(b, j):
        products = [one_tile(b, PER * j + s) for s in range(PER)]
        for k in range(RT):
            term = acc[b, k]
            for s in range(PER):
                slot = PER * j + s
                live = lists_s[b, 2, 0, slot].astype(jnp.float32)
                weight = jnp.where(lists_s[b, 0, 0, slot] == k, live, 0.0)
                term = term + weight * products[s]
            acc[b, k] = term

    def do_work(w, carry):
        @pl.when(w < 0)
        def _():
            for s in range(2):
                j = 2 * (w + HALF) + s
                pl.when(j < own_groups * HALF)(lambda: multiply(z, j))

        @pl.when(w >= 0)
        def _():
            for way in (0, 1):
                there, source, j = message(w, way)
                pl.when(there)(lambda: multiply(source, j))

        for i, when in ((0, -1), (1, 2 * HALF - 1), (-1, 2 * HALF - 1), (2, 4 * HALF - 1), (-2, 4 * HALF - 1)):
            pl.when(w == when)(lambda: near_copy(block(i)).start())
        return carry

    def block(i):
        return rem(z + i + NZ, NZ)

    def near_copy(b):
        return copy(
            acc.at[b, pl.ds((1 - core) * 8, 8)], near.at[b],
            near_send, near_recv.at[b], device(x, y, z, 1 - core),
        )

    def far_copy(b, step):
        there = rem(y + step, NY)
        return copy(
            acc.at[b, pl.ds(core * 8 + there * 2, 2)], far.at[b, step - 1],
            far_send, far_recv.at[b], device(x, there, z, core),
        )

    def pair_copy(b):
        return copy(
            acc.at[b, core * 8 + y * 2 + (1 - x_lo)], pair.at[b],
            pair_send, pair_recv.at[b], device(x_hi * 2 + 1 - x_lo, y, z, core),
        )

    mine = core * 8 + y * 2 + x_lo

    def out_copy(b, a):
        return copy(
            done.at[b, pl.ds(a * SHARE, SHARE)], out.at[:, pl.ds(pl.multiple_of(mine * TS, TS), TS)],
            out_send, out_recv, (x_hi * NZ + b, a * NZ + z),
        )

    def stage2(i):
        b = block(i)
        near_copy(b).wait_recv()

        @pl.loop(0, 8)
        def _(k):
            acc[b, core * 8 + k] = acc[b, core * 8 + k] + near[b, k]

        for step in (1, 2, 3):
            far_copy(b, step).start()

    def stage3(i):
        b = block(i)
        copy(far.at[b], far.at[b], far_send, far_recv.at[b], up).wait_recv()
        for k in range(2):
            place = core * 8 + y * 2 + k
            acc[b, place] = acc[b, place] + (far[b, 0, k] + far[b, 1, k] + far[b, 2, k])
        pair_copy(b).start()

    def is_home(b, a):
        return jnp.logical_and(b == z, a * NZ + z == col)

    def stage4(i):
        b = block(i)
        pair_copy(b).wait_recv()
        done[b] = acc[b, mine] + pair[b]
        for a in range(2):
            home = is_home(b, a)

            @pl.when(home)
            def _():
                out[:, pl.ds(pl.multiple_of(mine * TS, TS), TS)] = done[b, a * SHARE : (a + 1) * SHARE]

            @pl.when(jnp.logical_not(home))
            def _():
                out_copy(b, a).start()

    def prepare():
        all_lists.wait_recv()
        to_scalar = pltpu.make_async_copy(lists, lists_s, local_sem.at[0])
        to_scalar.start()
        for way in (0, 1):
            all_pieces(way)[1].wait_recv()

        @pl.loop(0, CT)
        def _(t):
            place = pl.ds(pl.multiple_of(t * TS, TS), TS)
            for a in range(2):
                value = both[a, :, place]
                high = value.astype(jnp.bfloat16)
                low = (value - high.astype(jnp.float32)).astype(jnp.bfloat16)
                split[t, a * SHARE : (a + 1) * SHARE] = high
                split[t, (2 + a) * SHARE : (3 + a) * SHARE] = low

        to_scalar.wait()

    def tick(t, worked):
        @pl.when(t < PIECES)
        def _():
            for way in (0, 1):
                hop1(way, t).wait_recv()
                hop2(way, t, relayed(way)).start()

        for way in (0, 1):
            arrive(t, way)
        pl.when(t == FIRST)(prepare)
        for stage, i, when in PLAN:
            pl.when(t == when)(lambda: (stage2, stage3, stage4)[stage - 2](i))
        stop = jnp.where(t < FIRST, worked, jnp.minimum(worked + MOST, t + 1))
        lax.fori_loop(worked, stop, do_work, 0)
        return stop

    lax.fori_loop(0, TICKS, tick, jnp.int32(-HALF))
    for i in (4, 3, -3):
        near_copy(block(i)).start()
    for stage, i in REST:
        (stage2, stage3, stage4)[stage - 2](i)

    homes = rem(col, NZ) == z

    @pl.when(homes)
    def _():
        part = out.at[:, pl.ds(0, (RT - 1) * TS)]
        copy(part, part, out_send, out_recv, up).wait()

    @pl.when(jnp.logical_not(homes))
    def _():
        copy(out, out, out_send, out_recv, up).wait()

    all_lists.wait_send()

    @pl.loop(0, TICKS)
    def _(k):
        for way in (0, 1):
            ring_sent(k, way)

    for way in (0, 1):
        for made in all_pieces(way):
            made.wait_send()
    copy(near, near, near_send, near_recv.at[0], up).wait_send()
    copy(far, far, far_send, far_recv.at[0], up).wait_send()
    copy(pair, pair, pair_send, pair_recv.at[0], up).wait_send()


def body(tile_values, tile_rows, tile_cols, tile_live, dense_factor):
    dma = pltpu.SemaphoreType.DMA
    vmem = pltpu.VMEM
    f32 = jnp.float32
    return pl.pallas_call(
        kernel,
        out_shape=jax.ShapeDtypeStruct((SHARE, RT * TS), f32),
        in_specs=[pl.BlockSpec(memory_space=pltpu.HBM)] * 5,
        out_specs=pl.BlockSpec(memory_space=pltpu.VMEM),
        scratch_shapes=[
            vmem((NZ, SLOTS, TS, TS), f32),
            vmem((NZ, 3, 1, SLOTS), jnp.int32),
            pltpu.SMEM((NZ, 3, 1, SLOTS), jnp.int32),
            vmem((2, PIECES, SHARE, SPAN), f32),
            vmem((2, SHARE, CT * TS), f32),
            vmem((CT, 4 * SHARE, TS), jnp.bfloat16),
            vmem((NZ, RT, 2 * SHARE, TS), f32),
            vmem((NZ, 8, 2 * SHARE, TS), f32),
            vmem((NZ, 3, 2, 2 * SHARE, TS), f32),
            vmem((NZ, 2 * SHARE, TS), f32),
            vmem((NZ, 2 * SHARE, TS), f32),
            dma((5,)),
            dma((TICKS,)), dma((TICKS,)), dma((TICKS,)), dma((TICKS,)),
            dma, dma,
            dma((2,)), dma((2, PIECES)), dma((2,)), dma((2,)),
            dma, dma((NZ,)), dma, dma((NZ,)), dma, dma((NZ,)), dma, dma,
        ],
        compiler_params=pltpu.CompilerParams(
            collective_id=0, has_side_effects=True, vmem_limit_bytes=67043328
        ),
    )(tile_values[0, 0], tile_rows[0], tile_cols[0], tile_live[0], dense_factor)


def solution(mesh):
    in_specs = (
        P("row", "col", None, None, None),
        P("row", "col", None),
        P("row", "col", None),
        P("row", "col", None),
        P("row", "col"),
    )
    out_specs = P("col", "row")
    return jax.shard_map(body, mesh=mesh, in_specs=in_specs, out_specs=out_specs, check_vma=False)
```

```python
import jax
import jax.numpy as jnp
from jax import lax
from jax.experimental import pallas as pl
from jax.experimental.pallas import tpu as pltpu
from jax.sharding import PartitionSpec as P

NX, NY, NZ = 4, 4, 8
TS = 128
SHARE = 32
RT = 16
CT = 64
SLOTS = 16
PER = 2
CHUNKS = SLOTS // PER
HALF = CHUNKS // 2
PIECES = 4
SPAN = CT * TS // (2 * PIECES)
GROUPS = 5
TICKS = GROUPS * HALF
NONE = 2 * GROUPS
FIRST = 7
MOST = 4
PLAN = (
    (2, 0, 9), (2, 1, 10), (2, -1, 11), (3, 0, 12), (3, 1, 13), (3, -1, 14),
    (4, 0, 15), (2, 2, 16), (2, -2, 16), (4, 1, 16), (4, -1, 17), (3, 2, 18),
)
MESH = pl.DeviceIdType.MESH


def rem(a, b):
    return lax.rem(a, jnp.int32(b))


def div(a, b):
    return lax.div(a, jnp.int32(b))


def kernel(
    tiles, rows_in, cols_in, live_in, dense, out,
    held, lists, lists_s, relay, both, split, acc, near, far, pair, done, across, beside, landing,
    local_sem,
    right_send, right_recv, left_send, left_recv, list_send, list_recv,
    hop1_send, hop1_recv, hop2_send, hop2_recv,
    near_send, near_recv, far_send, far_recv, pair_send, pair_recv, out_send, out_recv,
    across_send, across_recv, beside_send, beside_recv, halves_send,
):
    row, col = lax.axis_index("row"), lax.axis_index("col")
    x_hi, z = div(row, NZ), rem(row, NZ)
    y, x_lo, core = div(col, 4), rem(div(col, 2), 2), rem(col, 2)
    x = x_hi * 2 + x_lo

    def device(x, y, z, core):
        return (div(x, 2) * NZ + z, y * 4 + rem(x, 2) * 2 + core)

    def copy(src, dst, send_sem, recv_sem, target):
        return pltpu.make_async_remote_copy(
            src_ref=src, dst_ref=dst, send_sem=send_sem, recv_sem=recv_sem,
            device_id=target, device_id_type=MESH,
        )

    up = device(x, y, rem(z + 1, NZ), core)
    down = device(x, y, rem(z + NZ - 1, NZ), core)
    forth = device(rem(x + 1, NX), y, z, core)
    back = device(rem(x + NX - 1, NX), y, z, core)

    barrier = pltpu.get_barrier_semaphore()
    partners = [device(x, y, rem(z + step, NZ), core) for step in range(1, NZ)]
    partners += [forth, back, device(x, y, z, 1 - core)]
    partners += [device(x, rem(y + step, NY), z, core) for step in (1, 2, 3)]
    for partner in partners:
        pl.semaphore_signal(barrier, inc=1, device_id=partner, device_id_type=MESH)

    center = col - x_hi * NZ

    def banded(source):
        gap = source - center
        return jnp.logical_and(gap >= -1, gap <= 1)

    crossed = jnp.logical_and(center >= -1, center <= NZ)

    def place(source):
        return rem(source - center + 3 + 4 * NZ, NZ) - 3

    def hops(source, half, way):
        u = place(source)
        first = jnp.where(u > 0, 4, 3)
        second = jnp.where(u < 0, 2, jnp.where(u > 0, 5, 4))
        even = 3 + rem(source, 2)
        rightwards = jnp.where(crossed, jnp.where(half == 1, second, first), even)
        return rightwards if way == 0 else NZ - 1 - rightwards

    def half_of(source, turn, way):
        swap = (place(source) >= 0) if way == 0 else (place(source) < 0)
        return rem(turn + jnp.where(swap, 1, 0), 2)

    def travels(source, half, level, way):
        there = jnp.logical_or(half == 0, banded(source))
        return jnp.logical_and(there, level < hops(source, half, way))

    def source_of(level, way):
        return rem(z + 2 * NZ + (-level - 1 if way == 0 else level + 1), NZ)

    own_groups = jnp.where(banded(z), 2, 1)
    coming, passed, onward = [], [], []
    for way in (0, 1):
        group = [jnp.int32(NONE)] * GROUPS
        count = jnp.int32(0)
        for g in range(2 * GROUPS):
            source = source_of(g // 2, way)
            there = travels(source, half_of(source, g % 2, way), g // 2, way)
            for n in range(GROUPS):
                group[n] = jnp.where(jnp.logical_and(there, count == n), g, group[n])
            count = count + jnp.where(there, 1, 0)
        coming.append(group)
        goes, slots = [], []
        slot = own_groups
        for n in range(GROUPS):
            level = div(group[n], 2)
            source = source_of(level, way)
            on = travels(source, half_of(source, rem(group[n], 2), way), level + 1, way)
            on = jnp.logical_and(on, group[n] < NONE)
            goes.append(jnp.where(on, 1, 0))
            slots.append(slot)
            slot = slot + goes[-1]
        passed.append(goes)
        onward.append(slots)

    def pick(values, n):
        chosen = values[0]
        for i in range(1, GROUPS):
            chosen = jnp.where(n == i, values[i], chosen)
        return chosen

    def ring_copy(source, j, slot, way):
        part = held.at[source, pl.ds(PER * j, PER)]
        if way == 0:
            return copy(part, part, right_send.at[slot], right_recv.at[slot], up)
        return copy(part, part, left_send.at[slot], left_recv.at[slot], down)

    def message(t, way):
        group = pick(coming[way], div(t, HALF))
        source = source_of(div(group, 2), way)
        j = half_of(source, rem(group, 2), way) * HALF + rem(t, HALF)
        return group < NONE, source, j

    def arrive(t, way):
        there, source, j = message(t, way)

        @pl.when(there)
        def _():
            ring_copy(source, j, t, way).wait_recv()
            n = div(t, HALF)

            @pl.when(pick(passed[way], n) == 1)
            def _():
                ring_copy(source, j, pick(onward[way], n) * HALF + rem(t, HALF), way).start()

    def own_message(k, way):
        turn = div(k, HALF)
        half = jnp.where(own_groups == 2, half_of(z, turn, way), 0)
        return turn < own_groups, ring_copy(z, half * HALF + rem(k, HALF), k, way)

    def ring_sent(k, way):
        made = ring_copy(z, 0, k, way)
        slot = div(k, HALF)
        count = own_groups
        for n in range(GROUPS):
            count = count + passed[way][n]
        pl.when(slot < count)(made.wait_send)

    def list_copy(p):
        peer = rem(z + p, NZ)
        return copy(lists.at[z], lists.at[z], list_send, list_recv, device(x, y, peer, core))

    seven = lists.at[pl.ds(0, NZ - 1)]
    all_lists = copy(seven, seven, list_send, list_recv, up)

    def columns(way, k):
        return pl.ds(pl.multiple_of((way * PIECES + k) * SPAN, SPAN), SPAN)

    def hop1(way, k):
        return copy(
            both.at[x_hi, :, columns(way, k)], relay.at[way, k],
            hop1_send.at[way], hop1_recv.at[way, k], (forth, back)[way],
        )

    def hop2(way, k, owner):
        return copy(
            relay.at[way, k], both.at[owner, :, columns(way, k)],
            hop2_send.at[way], hop2_recv.at[way], (forth, back)[way],
        )

    def all_pieces(way):
        part = both.at[1 - x_hi, :, pl.ds(way * PIECES * SPAN, PIECES * SPAN)]
        return (
            copy(part, part, hop1_send.at[way], hop2_recv.at[way], forth),
            copy(part, part, hop2_send.at[way], hop2_recv.at[way], forth),
        )

    def relayed(way):
        return div(rem(x + (NX - 1 if way == 0 else 1), NX), 2)

    own_lists = [
        pltpu.make_async_copy(ref, lists.at[z, k], local_sem.at[k])
        for k, ref in enumerate((rows_in, cols_in, live_in))
    ]

    own_tiles = pltpu.make_async_copy(tiles, held.at[z], local_sem.at[3])
    own_dense = pltpu.make_async_copy(dense, both.at[x_hi], local_sem.at[4])
    for made in own_lists:
        made.start()
    own_tiles.start()
    own_dense.start()

    for made in own_lists:
        made.wait()
    own_tiles.wait()
    pl.semaphore_wait(barrier, len(partners))

    @pl.loop(1, NZ)
    def _(p):
        list_copy(p).start()

    @pl.loop(0, CHUNKS)
    def _(k):
        for way in (0, 1):
            there, made = own_message(k, way)
            pl.when(there)(made.start)

    own_dense.wait()

    @pl.loop(0, PIECES)
    def _(k):
        for way in (0, 1):
            hop1(way, k).start()

    @pl.loop(0, NZ * RT)
    def _(i):
        acc[div(i, RT), div(rem(i, RT), 8), div(rem(i, 8), 2), rem(i, 2)] = jnp.zeros(
            (2 * SHARE, TS), jnp.float32
        )

    def one_tile(b, slot):
        tile = held[b, slot]
        high = tile.astype(jnp.bfloat16)
        low = (tile - high.astype(jnp.float32)).astype(jnp.bfloat16)
        chosen = split[lists_s[b, 1, 0, slot]]
        dims = (((1,), (1,)), ((), ()))
        by_high = lax.dot_general(chosen, high, dims, preferred_element_type=jnp.float32)
        by_low = lax.dot_general(
            chosen[: 2 * SHARE], low, dims, preferred_element_type=jnp.float32
        )
        return by_high[: 2 * SHARE] + (by_high[2 * SHARE :] + by_low)

    def multiply(b, j):
        products = [one_tile(b, PER * j + s) for s in range(PER)]
        for k in range(RT):
            place_of = (b, k // 8, k // 2 % NY, k % 2)
            term = acc[place_of]
            for s in range(PER):
                slot = PER * j + s
                live = lists_s[b, 2, 0, slot].astype(jnp.float32)
                weight = jnp.where(lists_s[b, 0, 0, slot] == k, live, 0.0)
                term = term + weight * products[s]
            acc[place_of] = term

    def do_work(w, carry):
        @pl.when(w < 0)
        def _():
            for s in range(2):
                j = 2 * (w + HALF) + s
                pl.when(j < own_groups * HALF)(lambda: multiply(z, j))

        @pl.when(w >= 0)
        def _():
            for way in (0, 1):
                there, source, j = message(w, way)
                pl.when(there)(lambda: multiply(source, j))

        for i, when in ((0, -1), (1, 2 * HALF - 1), (-1, 2 * HALF - 1), (2, 4 * HALF - 1), (-2, 4 * HALF - 1)):
            pl.when(w == when)(lambda: near_copy(block(i)).start())
        return carry

    def block(i):
        return rem(z + i + NZ, NZ)

    def near_copy(b):
        return copy(
            acc.at[b, 1 - core], near.at[b],
            near_send, near_recv.at[b], device(x, y, z, 1 - core),
        )

    def far_copy(b, step):
        there = rem(y + step, NY)
        return copy(
            acc.at[b, core, there], far.at[b, step - 1],
            far_send, far_recv.at[b], device(x, there, z, core),
        )

    neighbour = device(x_hi * 2 + 1 - x_lo, y, z, core)

    def pair_copy(b):
        return copy(acc.at[b, core, y, 1 - x_lo], pair.at[b], pair_send, pair_recv.at[b], neighbour)

    def tile_row(k):
        return pl.ds(pl.multiple_of((core * 8 + y * 2 + k) * TS, TS), TS)

    def out_copy(b, a):
        return copy(
            done.at[b, pl.ds(a * SHARE, SHARE)], landing.at[0, :, tile_row(x_lo)],
            out_send, out_recv, (x_hi * NZ + b, a * NZ + z),
        )

    def is_home(b, a):
        return jnp.logical_and(b == z, a * NZ + z == col)

    def go_home(b):
        for a in range(2):
            home = is_home(b, a)

            @pl.when(home)
            def _():
                landing[0, :, tile_row(x_lo)] = done[b, a * SHARE : (a + 1) * SHARE]

            pl.when(jnp.logical_not(home))(out_copy(b, a).start)

    def take_near(b):
        near_copy(b).wait_recv()

        @pl.loop(0, 8)
        def _(k):
            spot = (b, core, div(k, 2), rem(k, 2))
            acc[spot] = acc[spot] + near[b, div(k, 2), rem(k, 2)]

    def take_far(b):
        copy(far.at[b], far.at[b], far_send, far_recv.at[b], up).wait_recv()
        for k in range(2):
            spot = (b, core, y, k)
            acc[spot] = acc[spot] + (far[b, 0, k] + far[b, 1, k] + far[b, 2, k])

    def stage2(i):
        b = block(i)
        take_near(b)
        for step in (1, 2, 3):
            far_copy(b, step).start()

    def stage3(i):
        b = block(i)
        take_far(b)
        pair_copy(b).start()

    def stage4(i):
        b = block(i)
        pair_copy(b).wait_recv()
        done[b] = acc[b, core, y, x_lo] + pair[b]
        go_home(b)

    def stage3_home(i):
        b = block(i)
        take_far(b)
        for k in range(2):
            for a in range(2):
                copy(
                    acc.at[b, core, y, k, pl.ds(a * SHARE, SHARE)], landing.at[x_lo, :, tile_row(k)],
                    halves_send, out_recv, (x_hi * NZ + b, a * NZ + z),
                ).start()

    def across_copy(b):
        return copy(acc.at[b, core, :, 1 - x_lo], across, across_send, across_recv, neighbour)

    def beside_copy(b, step):
        there = rem(y + step, NY)
        return copy(
            acc.at[b, core, there, x_lo], beside.at[step - 1],
            beside_send, beside_recv, device(x, there, z, core),
        )

    def stage2_across(i):
        b = block(i)
        take_near(b)
        across_copy(b).start()

    def stage3_across(i):
        b = block(i)
        across_copy(b).wait_recv()
        for k in range(NY):
            spot = (b, core, k, x_lo)
            acc[spot] = acc[spot] + across[k]
        for step in (1, 2, 3):
            beside_copy(b, step).start()

    def stage4_across(i):
        b = block(i)
        copy(beside, beside, beside_send, beside_recv, up).wait_recv()
        done[b] = acc[b, core, y, x_lo] + (beside[0] + beside[1] + beside[2])
        go_home(b)

    def prepare():
        all_lists.wait_recv()
        to_scalar = pltpu.make_async_copy(lists, lists_s, local_sem.at[0])
        to_scalar.start()
        for way in (0, 1):
            all_pieces(way)[1].wait_recv()

        @pl.loop(0, CT)
        def _(t):
            place = pl.ds(pl.multiple_of(t * TS, TS), TS)
            for a in range(2):
                value = both[a, :, place]
                high = value.astype(jnp.bfloat16)
                low = (value - high.astype(jnp.float32)).astype(jnp.bfloat16)
                split[t, a * SHARE : (a + 1) * SHARE] = high
                split[t, (2 + a) * SHARE : (3 + a) * SHARE] = low

        to_scalar.wait()

    def tick(t, worked):
        @pl.when(t < PIECES)
        def _():
            for way in (0, 1):
                hop1(way, t).wait_recv()
                hop2(way, t, relayed(way)).start()

        for way in (0, 1):
            arrive(t, way)
        pl.when(t == FIRST)(prepare)
        for stage, i, when in PLAN:
            pl.when(t == when)(lambda: (stage2, stage3, stage4)[stage - 2](i))
        stop = jnp.where(t < FIRST, worked, jnp.minimum(worked + MOST, t + 1))
        lax.fori_loop(worked, stop, do_work, 0)
        return stop

    lax.fori_loop(0, TICKS, tick, jnp.int32(-HALF))
    for i in (4, 3, -3):
        near_copy(block(i)).start()
    stage3(-2)
    stage4(2)
    stage2(4)
    stage2_across(3)
    stage2(-3)
    stage4(-2)
    stage3(4)
    stage3_across(3)
    stage4(4)
    stage3_home(-3)
    stage4_across(3)

    part = landing.at[0, :, pl.ds(0, 4 * TS)]
    copy(part, part, halves_send, out_recv, up).wait_send()
    across_copy(0).wait_send()
    copy(beside, beside, beside_send, beside_recv, up).wait_send()
    all_lists.wait_send()

    @pl.loop(0, TICKS)
    def _(k):
        for way in (0, 1):
            ring_sent(k, way)

    for way in (0, 1):
        for made in all_pieces(way):
            made.wait_send()
    copy(near, near, near_send, near_recv.at[0], up).wait_send()
    part = far.at[pl.ds(0, NZ - 1)]
    copy(part, part, far_send, far_recv.at[0], up).wait_send()
    part = pair.at[pl.ds(0, NZ - 2)]
    copy(part, part, pair_send, pair_recv.at[0], up).wait_send()

    way_home = rem(z - rem(col, NZ) + NZ, NZ)
    halved = way_home == NZ - 3
    homes = way_home == 0

    @pl.when(halved)
    def _():
        copy(landing, landing, out_send, out_recv, up).wait_recv()
        out[...] = landing[0] + landing[1]

    @pl.when(homes)
    def _():
        part = landing.at[0, :, pl.ds(0, (RT - 1) * TS)]
        copy(part, part, out_send, out_recv, up).wait_recv()
        part = landing.at[0, :, pl.ds(0, 13 * TS)]
        copy(part, part, out_send, out_recv, up).wait_send()

    @pl.when(jnp.logical_not(homes))
    def _():
        part = landing.at[0, :, pl.ds(0, 14 * TS)]
        copy(part, part, out_send, out_recv, up).wait_send()

    @pl.when(jnp.logical_not(jnp.logical_or(halved, homes)))
    def _():
        copy(landing.at[0], landing.at[0], out_send, out_recv, up).wait_recv()

    @pl.when(jnp.logical_not(halved))
    def _():
        out[...] = landing[0]


def body(tile_values, tile_rows, tile_cols, tile_live, dense_factor):
    dma = pltpu.SemaphoreType.DMA
    vmem = pltpu.VMEM
    f32 = jnp.float32
    return pl.pallas_call(
        kernel,
        out_shape=jax.ShapeDtypeStruct((SHARE, RT * TS), f32),
        in_specs=[pl.BlockSpec(memory_space=pltpu.HBM)] * 5,
        out_specs=pl.BlockSpec(memory_space=pltpu.VMEM),
        scratch_shapes=[
            vmem((NZ, SLOTS, TS, TS), f32),
            vmem((NZ, 3, 1, SLOTS), jnp.int32),
            pltpu.SMEM((NZ, 3, 1, SLOTS), jnp.int32),
            vmem((2, PIECES, SHARE, SPAN), f32),
            vmem((2, SHARE, CT * TS), f32),
            vmem((CT, 4 * SHARE, TS), jnp.bfloat16),
            vmem((NZ, 2, NY, 2, 2 * SHARE, TS), f32),
            vmem((NZ, NY, 2, 2 * SHARE, TS), f32),
            vmem((NZ, 3, 2, 2 * SHARE, TS), f32),
            vmem((NZ, 2 * SHARE, TS), f32),
            vmem((NZ, 2 * SHARE, TS), f32),
            vmem((NY, 2 * SHARE, TS), f32),
            vmem((3, 2 * SHARE, TS), f32),
            vmem((2, SHARE, RT * TS), f32),
            dma((5,)),
            dma((TICKS,)), dma((TICKS,)), dma((TICKS,)), dma((TICKS,)),
            dma, dma,
            dma((2,)), dma((2, PIECES)), dma((2,)), dma((2,)),
            dma, dma((NZ,)), dma, dma((NZ,)), dma, dma((NZ,)), dma, dma,
            dma, dma, dma, dma, dma,
        ],
        compiler_params=pltpu.CompilerParams(
            collective_id=0, has_side_effects=True, vmem_limit_bytes=67043328
        ),
    )(tile_values[0, 0], tile_rows[0], tile_cols[0], tile_live[0], dense_factor)


def solution(mesh):
    in_specs = (
        P("row", "col", None, None, None),
        P("row", "col", None),
        P("row", "col", None),
        P("row", "col", None),
        P("row", "col"),
    )
    out_specs = P("col", "row")
    return jax.shard_map(body, mesh=mesh, in_specs=in_specs, out_specs=out_specs, check_vma=False)
```

```python
import jax
import jax.numpy as jnp
from jax import lax
from jax.experimental import pallas as pl
from jax.experimental.pallas import tpu as pltpu
from jax.sharding import PartitionSpec as P

NX, NY, NZ = 4, 4, 8
TS = 128
SHARE = 32
RT = 16
CT = 64
SLOTS = 16
PER = 2
CHUNKS = SLOTS // PER
HALF = CHUNKS // 2
PIECES = 4
SPAN = CT * TS // (2 * PIECES)
GROUPS = 5
TICKS = GROUPS * HALF
NONE = 2 * GROUPS
FIRST = 7
MOST = 4
PLAN = (
    (2, 0, 9), (2, 1, 10), (2, -1, 11), (3, 0, 12), (3, 1, 13), (3, -1, 14),
    (4, 0, 15), (2, 2, 16), (2, -2, 16), (4, 1, 16), (4, -1, 17),
)
MESH = pl.DeviceIdType.MESH


def rem(a, b):
    return lax.rem(a, jnp.int32(b))


def div(a, b):
    return lax.div(a, jnp.int32(b))


def kernel(
    tiles, rows_in, cols_in, live_in, dense, out,
    held, lists, lists_s, relay, both, split, acc, near, far, pair, done, across, beside, landing,
    local_sem,
    right_send, right_recv, left_send, left_recv, list_send, list_recv,
    hop1_send, hop1_recv, hop2_send, hop2_recv,
    near_send, near_recv, far_send, far_recv, pair_send, pair_recv, out_send, out_recv,
    across_send, across_recv, beside_send, beside_recv, halves_send,
):
    row, col = lax.axis_index("row"), lax.axis_index("col")
    x_hi, z = div(row, NZ), rem(row, NZ)
    y, x_lo, core = div(col, 4), rem(div(col, 2), 2), rem(col, 2)
    x = x_hi * 2 + x_lo

    def device(x, y, z, core):
        return (div(x, 2) * NZ + z, y * 4 + rem(x, 2) * 2 + core)

    def copy(src, dst, send_sem, recv_sem, target):
        return pltpu.make_async_remote_copy(
            src_ref=src, dst_ref=dst, send_sem=send_sem, recv_sem=recv_sem,
            device_id=target, device_id_type=MESH,
        )

    up = device(x, y, rem(z + 1, NZ), core)
    down = device(x, y, rem(z + NZ - 1, NZ), core)
    forth = device(rem(x + 1, NX), y, z, core)
    back = device(rem(x + NX - 1, NX), y, z, core)

    barrier = pltpu.get_barrier_semaphore()
    partners = [device(x, y, rem(z + step, NZ), core) for step in range(1, NZ)]
    partners += [forth, back, device(x, y, z, 1 - core)]
    partners += [device(x, rem(y + step, NY), z, core) for step in (1, 2, 3)]
    for partner in partners:
        pl.semaphore_signal(barrier, inc=1, device_id=partner, device_id_type=MESH)

    center = col - x_hi * NZ

    def banded(source):
        gap = source - center
        return jnp.logical_and(gap >= -1, gap <= 1)

    both_of = jnp.logical_and
    crossed = jnp.logical_and(center >= -1, center <= NZ)

    def place(source):
        return rem(source - center + 3 + 4 * NZ, NZ) - 3

    def hops(source, half, way):
        u = place(source)
        first = jnp.where(u > 0, 4, 3)
        second = jnp.where(u < 0, 2, jnp.where(u > 0, 5, 4))
        even = 3 + rem(source, 2)
        rightwards = jnp.where(crossed, jnp.where(half == 1, second, first), even)
        return rightwards if way == 0 else NZ - 1 - rightwards

    def half_of(source, turn, way):
        swap = (place(source) >= 0) if way == 0 else (place(source) < 0)
        return rem(turn + jnp.where(swap, 1, 0), 2)

    def travels(source, half, level, way):
        there = jnp.logical_or(half == 0, banded(source))
        return jnp.logical_and(there, level < hops(source, half, way))

    def source_of(level, way):
        return rem(z + 2 * NZ + (-level - 1 if way == 0 else level + 1), NZ)

    own_groups = jnp.where(banded(z), 2, 1)
    coming, passed, onward = [], [], []
    for way in (0, 1):
        group = [jnp.int32(NONE)] * GROUPS
        count = jnp.int32(0)
        for g in range(2 * GROUPS):
            source = source_of(g // 2, way)
            there = travels(source, half_of(source, g % 2, way), g // 2, way)
            for n in range(GROUPS):
                group[n] = jnp.where(jnp.logical_and(there, count == n), g, group[n])
            count = count + jnp.where(there, 1, 0)
        coming.append(group)
        goes, slots = [], []
        slot = own_groups
        for n in range(GROUPS):
            level = div(group[n], 2)
            source = source_of(level, way)
            on = travels(source, half_of(source, rem(group[n], 2), way), level + 1, way)
            on = jnp.logical_and(on, group[n] < NONE)
            goes.append(jnp.where(on, 1, 0))
            slots.append(slot)
            slot = slot + goes[-1]
        passed.append(goes)
        onward.append(slots)

    def pick(values, n):
        chosen = values[0]
        for i in range(1, GROUPS):
            chosen = jnp.where(n == i, values[i], chosen)
        return chosen

    def ring_copy(source, j, slot, way):
        part = held.at[source, pl.ds(PER * j, PER)]
        if way == 0:
            return copy(part, part, right_send, right_recv.at[slot], up)
        return copy(part, part, left_send, left_recv.at[slot], down)

    def message(t, way):
        group = pick(coming[way], div(t, HALF))
        source = source_of(div(group, 2), way)
        j = half_of(source, rem(group, 2), way) * HALF + rem(t, HALF)
        return group < NONE, source, j

    def arrive(t, way):
        there, source, j = message(t, way)

        @pl.when(there)
        def _():
            ring_copy(source, j, t, way).wait_recv()
            n = div(t, HALF)

            @pl.when(pick(passed[way], n) == 1)
            def _():
                ring_copy(source, j, pick(onward[way], n) * HALF + rem(t, HALF), way).start()

    def own_message(k, way):
        turn = div(k, HALF)
        half = jnp.where(own_groups == 2, half_of(z, turn, way), 0)
        return turn < own_groups, ring_copy(z, half * HALF + rem(k, HALF), k, way)

    def ring_sent(way):
        count = own_groups
        for n in range(GROUPS):
            count = count + passed[way][n]
        for c in range(1, GROUPS + 1):
            part = held.at[pl.ds(0, c), pl.ds(0, PER * HALF)]
            sem = right_send if way == 0 else left_send
            pl.when(count == c)(copy(part, part, sem, right_recv.at[0], up).wait_send)

    def list_copy(p):
        peer = rem(z + p, NZ)
        return copy(lists.at[z], lists.at[z], list_send, list_recv, device(x, y, peer, core))

    seven = lists.at[pl.ds(0, NZ - 1)]
    all_lists = copy(seven, seven, list_send, list_recv, up)

    def columns(way, k):
        return pl.ds(pl.multiple_of((way * PIECES + k) * SPAN, SPAN), SPAN)

    def hop1(way, k):
        return copy(
            both.at[x_hi, :, columns(way, k)], relay.at[way, k],
            hop1_send.at[way], hop1_recv.at[way, k], (forth, back)[way],
        )

    def hop2(way, k, owner):
        return copy(
            relay.at[way, k], both.at[owner, :, columns(way, k)],
            hop2_send.at[way], hop2_recv.at[way], (forth, back)[way],
        )

    def all_pieces(way):
        part = both.at[1 - x_hi, :, pl.ds(way * PIECES * SPAN, PIECES * SPAN)]
        return (
            copy(part, part, hop1_send.at[way], hop2_recv.at[way], forth),
            copy(part, part, hop2_send.at[way], hop2_recv.at[way], forth),
        )

    def relayed(way):
        return div(rem(x + (NX - 1 if way == 0 else 1), NX), 2)

    own_lists = [
        pltpu.make_async_copy(ref, lists.at[z, k], local_sem.at[k])
        for k, ref in enumerate((rows_in, cols_in, live_in))
    ]

    own_tiles = pltpu.make_async_copy(tiles, held.at[z], local_sem.at[3])
    own_dense = pltpu.make_async_copy(dense, both.at[x_hi], local_sem.at[4])
    for made in own_lists:
        made.start()
    own_tiles.start()
    own_dense.start()

    for made in own_lists:
        made.wait()
    own_tiles.wait()
    pl.semaphore_wait(barrier, len(partners))

    @pl.loop(1, NZ)
    def _(p):
        list_copy(p).start()

    @pl.loop(0, CHUNKS)
    def _(k):
        for way in (0, 1):
            there, made = own_message(k, way)
            pl.when(there)(made.start)

    own_dense.wait()

    @pl.loop(0, PIECES)
    def _(k):
        for way in (0, 1):
            hop1(way, k).start()

    @pl.loop(0, NZ * RT)
    def _(i):
        acc[div(i, RT), div(rem(i, RT), 8), div(rem(i, 8), 2), rem(i, 2)] = jnp.zeros(
            (2 * SHARE, TS), jnp.float32
        )

    def one_tile(b, slot):
        tile = held[b, slot]
        high = tile.astype(jnp.bfloat16)
        low = (tile - high.astype(jnp.float32)).astype(jnp.bfloat16)
        chosen = split[lists_s[b, 1, 0, slot]]
        dims = (((1,), (1,)), ((), ()))
        by_high = lax.dot_general(chosen, high, dims, preferred_element_type=jnp.float32)
        by_low = lax.dot_general(
            chosen[: 2 * SHARE], low, dims, preferred_element_type=jnp.float32
        )
        return by_high[: 2 * SHARE] + (by_high[2 * SHARE :] + by_low)

    def multiply(*messages):
        products = [[one_tile(b, PER * j + s) for s in range(PER)] for b, j in messages]
        for (b, j), pair_of in zip(messages, products):
            slots = [PER * j + s for s in range(PER)]
            lives = [lists_s[b, 2, 0, slot].astype(jnp.float32) for slot in slots]
            for k in range(RT):
                place_of = (b, k // 8, k // 2 % NY, k % 2)
                term = acc[place_of]
                for s in range(PER):
                    weight = jnp.where(lists_s[b, 0, 0, slots[s]] == k, lives[s], 0.0)
                    term = term + weight * pair_of[s]
                acc[place_of] = term

    def do_work(w, carry):
        @pl.when(both_of(w < 0, 2 * (w + HALF) < own_groups * HALF))
        def _():
            multiply((z, 2 * (w + HALF)), (z, 2 * (w + HALF) + 1))

        @pl.when(w >= 0)
        def _():
            there, source, j = message(w, 0)
            there_too, source_too, j_too = message(w, 1)
            pl.when(both_of(there, there_too))(lambda: multiply((source, j), (source_too, j_too)))
            alone, alone_j = jnp.where(there, source, source_too), jnp.where(there, j, j_too)
            pl.when(there != there_too)(lambda: multiply((alone, alone_j)))

        for i, when in ((0, -1), (1, 2 * HALF - 1), (-1, 2 * HALF - 1), (2, 4 * HALF - 1), (-2, 4 * HALF - 1)):
            pl.when(w == when)(lambda: near_copy(block(i)).start())
        return carry

    def block(i):
        return rem(z + i + NZ, NZ)

    def near_copy(b):
        return copy(
            acc.at[b, 1 - core], near.at[b],
            near_send, near_recv.at[b], device(x, y, z, 1 - core),
        )

    def far_copy(b, step):
        there = rem(y + step, NY)
        return copy(
            acc.at[b, core, there], far.at[b, step - 1],
            far_send, far_recv.at[b], device(x, there, z, core),
        )

    neighbour = device(x_hi * 2 + 1 - x_lo, y, z, core)

    def pair_copy(b):
        return copy(acc.at[b, core, y, 1 - x_lo], pair.at[b], pair_send, pair_recv.at[b], neighbour)

    def tile_row(k):
        return pl.ds(pl.multiple_of((core * 8 + y * 2 + k) * TS, TS), TS)

    def out_copy(b, a):
        return copy(
            done.at[b, pl.ds(a * SHARE, SHARE)], landing.at[0, :, tile_row(x_lo)],
            out_send, out_recv, (x_hi * NZ + b, a * NZ + z),
        )

    def is_home(b, a):
        return jnp.logical_and(b == z, a * NZ + z == col)

    def go_home(b):
        for a in range(2):
            home = is_home(b, a)

            @pl.when(home)
            def _():
                landing[0, :, tile_row(x_lo)] = done[b, a * SHARE : (a + 1) * SHARE]

            pl.when(jnp.logical_not(home))(out_copy(b, a).start)

    def take_near(b):
        near_copy(b).wait_recv()

        @pl.loop(0, 8)
        def _(k):
            spot = (b, core, div(k, 2), rem(k, 2))
            acc[spot] = acc[spot] + near[b, div(k, 2), rem(k, 2)]

    def take_far(b):
        copy(far.at[b], far.at[b], far_send, far_recv.at[b], up).wait_recv()
        for k in range(2):
            spot = (b, core, y, k)
            acc[spot] = acc[spot] + (far[b, 0, k] + far[b, 1, k] + far[b, 2, k])

    def stage2(i):
        b = block(i)
        take_near(b)
        for step in (1, 2, 3):
            far_copy(b, step).start()

    def stage3(i):
        b = block(i)
        take_far(b)
        pair_copy(b).start()

    def stage4(i):
        b = block(i)
        pair_copy(b).wait_recv()
        done[b] = acc[b, core, y, x_lo] + pair[b]
        go_home(b)

    def stage3_home(i):
        b = block(i)
        take_far(b)
        for k in range(2):
            for a in range(2):
                copy(
                    acc.at[b, core, y, k, pl.ds(a * SHARE, SHARE)], landing.at[x_lo, :, tile_row(k)],
                    halves_send, out_recv, (x_hi * NZ + b, a * NZ + z),
                ).start()

    def across_copy(b):
        return copy(acc.at[b, core, :, 1 - x_lo], across, across_send, across_recv, neighbour)

    def beside_copy(b, step):
        there = rem(y + step, NY)
        return copy(
            acc.at[b, core, there, x_lo], beside.at[step - 1],
            beside_send, beside_recv, device(x, there, z, core),
        )

    def stage2_across(i):
        b = block(i)
        take_near(b)
        across_copy(b).start()

    def stage3_across(i):
        b = block(i)
        across_copy(b).wait_recv()
        for k in range(NY):
            spot = (b, core, k, x_lo)
            acc[spot] = acc[spot] + across[k]
        for step in (1, 2, 3):
            beside_copy(b, step).start()

    def stage4_across(i):
        b = block(i)
        copy(beside, beside, beside_send, beside_recv, up).wait_recv()
        done[b] = acc[b, core, y, x_lo] + (beside[0] + beside[1] + beside[2])
        go_home(b)

    def prepare():
        all_lists.wait_recv()
        to_scalar = pltpu.make_async_copy(lists, lists_s, local_sem.at[0])
        to_scalar.start()
        for way in (0, 1):
            all_pieces(way)[1].wait_recv()

        @pl.loop(0, CT)
        def _(t):
            place = pl.ds(pl.multiple_of(t * TS, TS), TS)
            for a in range(2):
                value = both[a, :, place]
                high = value.astype(jnp.bfloat16)
                low = (value - high.astype(jnp.float32)).astype(jnp.bfloat16)
                split[t, a * SHARE : (a + 1) * SHARE] = high
                split[t, (2 + a) * SHARE : (3 + a) * SHARE] = low

        to_scalar.wait()

    def tick(t, worked):
        @pl.when(t < PIECES)
        def _():
            for way in (0, 1):
                hop1(way, t).wait_recv()
                hop2(way, t, relayed(way)).start()

        for way in (0, 1):
            arrive(t, way)
        pl.when(t == FIRST)(prepare)
        for stage, i, when in PLAN:
            pl.when(t == when)(lambda: (stage2, stage3, stage4)[stage - 2](i))
        stop = jnp.where(t < FIRST, worked, jnp.minimum(worked + MOST, t + 1))
        lax.fori_loop(worked, stop, do_work, 0)
        return stop

    lax.fori_loop(0, TICKS, tick, jnp.int32(-HALF))
    for i in (4, 3, -3):
        near_copy(block(i)).start()
    stage3(2)
    stage3(-2)
    stage2(4)
    stage2_across(3)
    stage2(-3)
    stage4(2)
    stage4(-2)
    stage3(4)
    stage3_across(3)
    stage4(4)
    stage3_home(-3)
    stage4_across(3)

    part = landing.at[0, :, pl.ds(0, 4 * TS)]
    copy(part, part, halves_send, out_recv, up).wait_send()
    across_copy(0).wait_send()
    copy(beside, beside, beside_send, beside_recv, up).wait_send()
    all_lists.wait_send()

    for way in (0, 1):
        ring_sent(way)

    for way in (0, 1):
        for made in all_pieces(way):
            made.wait_send()
    copy(near, near, near_send, near_recv.at[0], up).wait_send()
    part = far.at[pl.ds(0, NZ - 1)]
    copy(part, part, far_send, far_recv.at[0], up).wait_send()
    part = pair.at[pl.ds(0, NZ - 2)]
    copy(part, part, pair_send, pair_recv.at[0], up).wait_send()

    way_home = rem(z - rem(col, NZ) + NZ, NZ)
    halved = way_home == NZ - 3
    homes = way_home == 0

    @pl.when(halved)
    def _():
        copy(landing, landing, out_send, out_recv, up).wait_recv()
        out[...] = landing[0] + landing[1]

    @pl.when(homes)
    def _():
        part = landing.at[0, :, pl.ds(0, (RT - 1) * TS)]
        copy(part, part, out_send, out_recv, up).wait_recv()
        part = landing.at[0, :, pl.ds(0, 13 * TS)]
        copy(part, part, out_send, out_recv, up).wait_send()

    @pl.when(jnp.logical_not(homes))
    def _():
        part = landing.at[0, :, pl.ds(0, 14 * TS)]
        copy(part, part, out_send, out_recv, up).wait_send()

    @pl.when(jnp.logical_not(jnp.logical_or(halved, homes)))
    def _():
        copy(landing.at[0], landing.at[0], out_send, out_recv, up).wait_recv()

    @pl.when(jnp.logical_not(halved))
    def _():
        out[...] = landing[0]


def body(tile_values, tile_rows, tile_cols, tile_live, dense_factor):
    dma = pltpu.SemaphoreType.DMA
    vmem = pltpu.VMEM
    f32 = jnp.float32
    return pl.pallas_call(
        kernel,
        out_shape=jax.ShapeDtypeStruct((SHARE, RT * TS), f32),
        in_specs=[pl.BlockSpec(memory_space=pltpu.HBM)] * 5,
        out_specs=pl.BlockSpec(memory_space=pltpu.VMEM),
        scratch_shapes=[
            vmem((NZ, SLOTS, TS, TS), f32),
            vmem((NZ, 3, 1, SLOTS), jnp.int32),
            pltpu.SMEM((NZ, 3, 1, SLOTS), jnp.int32),
            vmem((2, PIECES, SHARE, SPAN), f32),
            vmem((2, SHARE, CT * TS), f32),
            vmem((CT, 4 * SHARE, TS), jnp.bfloat16),
            vmem((NZ, 2, NY, 2, 2 * SHARE, TS), f32),
            vmem((NZ, NY, 2, 2 * SHARE, TS), f32),
            vmem((NZ, 3, 2, 2 * SHARE, TS), f32),
            vmem((NZ, 2 * SHARE, TS), f32),
            vmem((NZ, 2 * SHARE, TS), f32),
            vmem((NY, 2 * SHARE, TS), f32),
            vmem((3, 2 * SHARE, TS), f32),
            vmem((2, SHARE, RT * TS), f32),
            dma((5,)),
            dma, dma((TICKS,)), dma, dma((TICKS,)),
            dma, dma,
            dma((2,)), dma((2, PIECES)), dma((2,)), dma((2,)),
            dma, dma((NZ,)), dma, dma((NZ,)), dma, dma((NZ,)), dma, dma,
            dma, dma, dma, dma, dma,
        ],
        compiler_params=pltpu.CompilerParams(
            collective_id=0, has_side_effects=True, vmem_limit_bytes=56000000
        ),
    )(tile_values[0, 0], tile_rows[0], tile_cols[0], tile_live[0], dense_factor)


def solution(mesh):
    in_specs = (
        P("row", "col", None, None, None),
        P("row", "col", None),
        P("row", "col", None),
        P("row", "col", None),
        P("row", "col"),
    )
    out_specs = P("col", "row")
    return jax.shard_map(body, mesh=mesh, in_specs=in_specs, out_specs=out_specs, check_vma=False)
```

```python
import jax
import jax.numpy as jnp
from jax import lax
from jax.experimental import pallas as pl
from jax.experimental.pallas import tpu as pltpu
from jax.sharding import PartitionSpec as P

NX, NY, NZ = 4, 4, 8
TS = 128
SHARE = 32
RT = 16
CT = 64
SLOTS = 16
PER = 2
CHUNKS = SLOTS // PER
HALF = CHUNKS // 2
PIECES = 4
SPAN = CT * TS // (2 * PIECES)
GROUPS = 5
TICKS = GROUPS * HALF
NONE = 2 * GROUPS
LAST = 17
FIRST = 7
MOST = 4
PLAN = (
    (2, 0, 9), (2, 1, 10), (2, -1, 11), (3, 0, 12), (3, 1, 13), (3, -1, 14),
    (4, 0, 15), (4, 1, 16), (2, 2, 16), (2, -2, 17), (4, -1, 17),
)
MESH = pl.DeviceIdType.MESH


def rem(a, b):
    return lax.rem(a, jnp.int32(b))


def div(a, b):
    return lax.div(a, jnp.int32(b))


def kernel(
    tiles, rows_in, cols_in, live_in, dense, out,
    held, lists, lists_s, relay, both, split, acc, near, far, pair, done, across, beside, landing,
    local_sem,
    right_send, right_recv, left_send, left_recv, list_send, list_recv,
    hop1_send, hop1_recv, hop2_send, hop2_recv,
    near_send, near_recv, far_send, far_recv, pair_send, pair_recv, out_send, out_recv,
    across_send, across_recv, beside_send, beside_recv, halves_send,
):
    row, col = lax.axis_index("row"), lax.axis_index("col")
    x_hi, z = div(row, NZ), rem(row, NZ)
    y, x_lo, core = div(col, 4), rem(div(col, 2), 2), rem(col, 2)
    x = x_hi * 2 + x_lo

    def device(x, y, z, core):
        return (div(x, 2) * NZ + z, y * 4 + rem(x, 2) * 2 + core)

    def copy(src, dst, send_sem, recv_sem, target):
        return pltpu.make_async_remote_copy(
            src_ref=src, dst_ref=dst, send_sem=send_sem, recv_sem=recv_sem,
            device_id=target, device_id_type=MESH,
        )

    up = device(x, y, rem(z + 1, NZ), core)
    down = device(x, y, rem(z + NZ - 1, NZ), core)
    forth = device(rem(x + 1, NX), y, z, core)
    back = device(rem(x + NX - 1, NX), y, z, core)

    barrier = pltpu.get_barrier_semaphore()
    partners = [device(x, y, rem(z + step, NZ), core) for step in range(1, NZ)]
    partners += [forth, back, device(x, y, z, 1 - core)]
    partners += [device(x, rem(y + step, NY), z, core) for step in (1, 2, 3)]
    for partner in partners:
        pl.semaphore_signal(barrier, inc=1, device_id=partner, device_id_type=MESH)

    center = col - x_hi * NZ

    def banded(source):
        gap = source - center
        return jnp.logical_and(gap >= -1, gap <= 1)

    both_of = jnp.logical_and
    crossed = jnp.logical_and(center >= -1, center <= NZ)

    def place(source):
        return rem(source - center + 3 + 4 * NZ, NZ) - 3

    def hops(source, half, way):
        u = place(source)
        first = jnp.where(u > 0, 4, 3)
        second = jnp.where(u < 0, 2, jnp.where(u > 0, 5, 4))
        even = 3 + rem(source, 2)
        rightwards = jnp.where(crossed, jnp.where(half == 1, second, first), even)
        return rightwards if way == 0 else NZ - 1 - rightwards

    def half_of(source, turn, way):
        swap = (place(source) >= 0) if way == 0 else (place(source) < 0)
        return rem(turn + jnp.where(swap, 1, 0), 2)

    def travels(source, half, level, way):
        there = jnp.logical_or(half == 0, banded(source))
        return jnp.logical_and(there, level < hops(source, half, way))

    def source_of(level, way):
        return rem(z + 2 * NZ + (-level - 1 if way == 0 else level + 1), NZ)

    own_groups = jnp.where(banded(z), 2, 1)
    coming, passed, onward = [], [], []
    for way in (0, 1):
        group = [jnp.int32(NONE)] * GROUPS
        count = jnp.int32(0)
        for g in range(2 * GROUPS):
            source = source_of(g // 2, way)
            there = travels(source, half_of(source, g % 2, way), g // 2, way)
            for n in range(GROUPS):
                group[n] = jnp.where(jnp.logical_and(there, count == n), g, group[n])
            count = count + jnp.where(there, 1, 0)
        coming.append(group)
        goes, slots = [], []
        slot = own_groups
        for n in range(GROUPS):
            level = div(group[n], 2)
            source = source_of(level, way)
            on = travels(source, half_of(source, rem(group[n], 2), way), level + 1, way)
            on = jnp.logical_and(on, group[n] < NONE)
            goes.append(jnp.where(on, 1, 0))
            slots.append(slot)
            slot = slot + goes[-1]
        passed.append(goes)
        onward.append(slots)

    def pick(values, n):
        chosen = values[0]
        for i in range(1, GROUPS):
            chosen = jnp.where(n == i, values[i], chosen)
        return chosen

    def ring_copy(source, j, slot, way):
        part = held.at[source, pl.ds(PER * j, PER)]
        if way == 0:
            return copy(part, part, right_send, right_recv.at[slot], up)
        return copy(part, part, left_send, left_recv.at[slot], down)

    def message(t, way):
        group = pick(coming[way], div(t, HALF))
        source = source_of(div(group, 2), way)
        j = half_of(source, rem(group, 2), way) * HALF + rem(t, HALF)
        return group < NONE, source, j

    def arrive(t, way):
        there, source, j = message(t, way)

        @pl.when(there)
        def _():
            ring_copy(source, j, t, way).wait_recv()
            n = div(t, HALF)

            @pl.when(pick(passed[way], n) == 1)
            def _():
                ring_copy(source, j, pick(onward[way], n) * HALF + rem(t, HALF), way).start()

    def own_message(k, way):
        turn = div(k, HALF)
        half = jnp.where(own_groups == 2, half_of(z, turn, way), 0)
        return turn < own_groups, ring_copy(z, half * HALF + rem(k, HALF), k, way)

    def ring_sent(way):
        count = own_groups
        for n in range(GROUPS):
            count = count + passed[way][n]
        for c in range(1, GROUPS + 1):
            part = held.at[pl.ds(0, c), pl.ds(0, PER * HALF)]
            sem = right_send if way == 0 else left_send
            pl.when(count == c)(copy(part, part, sem, right_recv.at[0], up).wait_send)

    def list_copy(p):
        peer = rem(z + p, NZ)
        return copy(lists.at[z], lists.at[z], list_send, list_recv, device(x, y, peer, core))

    seven = lists.at[pl.ds(0, NZ - 1)]
    all_lists = copy(seven, seven, list_send, list_recv, up)

    def columns(way, k):
        return pl.ds(pl.multiple_of((way * PIECES + k) * SPAN, SPAN), SPAN)

    def hop1(way, k):
        return copy(
            both.at[x_hi, :, columns(way, k)], relay.at[way, k],
            hop1_send.at[way], hop1_recv.at[way, k], (forth, back)[way],
        )

    def hop2(way, k, owner):
        return copy(
            relay.at[way, k], both.at[owner, :, columns(way, k)],
            hop2_send.at[way], hop2_recv.at[way], (forth, back)[way],
        )

    def all_pieces(way):
        part = both.at[1 - x_hi, :, pl.ds(way * PIECES * SPAN, PIECES * SPAN)]
        return (
            copy(part, part, hop1_send.at[way], hop2_recv.at[way], forth),
            copy(part, part, hop2_send.at[way], hop2_recv.at[way], forth),
        )

    def relayed(way):
        return div(rem(x + (NX - 1 if way == 0 else 1), NX), 2)

    own_lists = [
        pltpu.make_async_copy(ref, lists.at[z, k], local_sem.at[k])
        for k, ref in enumerate((rows_in, cols_in, live_in))
    ]

    own_tiles = pltpu.make_async_copy(tiles, held.at[z], local_sem.at[3])
    own_dense = pltpu.make_async_copy(dense, both.at[x_hi], local_sem.at[4])
    for made in own_lists:
        made.start()
    own_tiles.start()
    own_dense.start()

    for made in own_lists:
        made.wait()
    own_tiles.wait()
    pl.semaphore_wait(barrier, len(partners))

    @pl.loop(1, NZ)
    def _(p):
        list_copy(p).start()

    @pl.loop(0, CHUNKS)
    def _(k):
        for way in (0, 1):
            there, made = own_message(k, way)
            pl.when(there)(made.start)

    own_dense.wait()

    @pl.loop(0, PIECES)
    def _(k):
        for way in (0, 1):
            hop1(way, k).start()

    @pl.loop(0, NZ * RT)
    def _(i):
        acc[div(i, RT), div(rem(i, RT), 8), div(rem(i, 8), 2), rem(i, 2)] = jnp.zeros(
            (2 * SHARE, TS), jnp.float32
        )

    def one_tile(b, slot):
        tile = held[b, slot]
        high = tile.astype(jnp.bfloat16)
        low = (tile - high.astype(jnp.float32)).astype(jnp.bfloat16)
        chosen = split[lists_s[b, 1, 0, slot]]
        dims = (((1,), (1,)), ((), ()))
        by_high = lax.dot_general(chosen, high, dims, preferred_element_type=jnp.float32)
        by_low = lax.dot_general(
            chosen[: 2 * SHARE], low, dims, preferred_element_type=jnp.float32
        )
        return by_high[: 2 * SHARE] + (by_high[2 * SHARE :] + by_low)

    def multiply(*messages):
        products = [[one_tile(b, PER * j + s) for s in range(PER)] for b, j in messages]
        for (b, j), pair_of in zip(messages, products):
            slots = [PER * j + s for s in range(PER)]
            lives = [lists_s[b, 2, 0, slot].astype(jnp.float32) for slot in slots]
            for k in range(RT):
                place_of = (b, k // 8, k // 2 % NY, k % 2)
                term = acc[place_of]
                for s in range(PER):
                    weight = jnp.where(lists_s[b, 0, 0, slots[s]] == k, lives[s], 0.0)
                    term = term + weight * pair_of[s]
                acc[place_of] = term

    def do_work(w, carry):
        @pl.when(both_of(w < 0, 2 * (w + HALF) < own_groups * HALF))
        def _():
            multiply((z, 2 * (w + HALF)), (z, 2 * (w + HALF) + 1))

        @pl.when(w >= 0)
        def _():
            there, source, j = message(w, 0)
            there_too, source_too, j_too = message(w, 1)
            pl.when(both_of(there, there_too))(lambda: multiply((source, j), (source_too, j_too)))
            alone, alone_j = jnp.where(there, source, source_too), jnp.where(there, j, j_too)
            pl.when(there != there_too)(lambda: multiply((alone, alone_j)))

        for i, when in ((0, -1), (1, 2 * HALF - 1), (-1, 2 * HALF - 1), (2, 4 * HALF - 1), (-2, 4 * HALF - 1)):
            pl.when(w == when)(lambda: near_copy(block(i)).start())
        return carry

    def block(i):
        return rem(z + i + NZ, NZ)

    def near_copy(b):
        return copy(
            acc.at[b, 1 - core], near.at[b],
            near_send, near_recv.at[b], device(x, y, z, 1 - core),
        )

    def far_copy(b, step):
        there = rem(y + step, NY)
        return copy(
            acc.at[b, core, there], far.at[b, step - 1],
            far_send, far_recv.at[b], device(x, there, z, core),
        )

    neighbour = device(x_hi * 2 + 1 - x_lo, y, z, core)

    def pair_copy(b):
        return copy(acc.at[b, core, y, 1 - x_lo], pair.at[b], pair_send, pair_recv.at[b], neighbour)

    def tile_row(k):
        return pl.ds(pl.multiple_of((core * 8 + y * 2 + k) * TS, TS), TS)

    def out_copy(b, a):
        return copy(
            done.at[b, pl.ds(a * SHARE, SHARE)], landing.at[0, :, tile_row(x_lo)],
            out_send, out_recv, (x_hi * NZ + b, a * NZ + z),
        )

    def is_home(b, a):
        return jnp.logical_and(b == z, a * NZ + z == col)

    def go_home(b):
        for a in range(2):
            home = is_home(b, a)

            @pl.when(home)
            def _():
                landing[0, :, tile_row(x_lo)] = done[b, a * SHARE : (a + 1) * SHARE]

            pl.when(jnp.logical_not(home))(out_copy(b, a).start)

    def take_near(b):
        near_copy(b).wait_recv()

        @pl.loop(0, 8)
        def _(k):
            spot = (b, core, div(k, 2), rem(k, 2))
            acc[spot] = acc[spot] + near[b, div(k, 2), rem(k, 2)]

    def take_far(b):
        copy(far.at[b], far.at[b], far_send, far_recv.at[b], up).wait_recv()
        for k in range(2):
            spot = (b, core, y, k)
            acc[spot] = acc[spot] + (far[b, 0, k] + far[b, 1, k] + far[b, 2, k])

    def stage2(i):
        b = block(i)
        take_near(b)
        for step in (1, 2, 3):
            far_copy(b, step).start()

    def stage3(i):
        b = block(i)
        take_far(b)
        pair_copy(b).start()

    def stage4(i):
        b = block(i)
        pair_copy(b).wait_recv()
        done[b] = acc[b, core, y, x_lo] + pair[b]
        go_home(b)

    def stage3_home(i):
        b = block(i)
        take_far(b)
        for k in range(2):
            for a in range(2):
                copy(
                    acc.at[b, core, y, k, pl.ds(a * SHARE, SHARE)], landing.at[x_lo, :, tile_row(k)],
                    halves_send, out_recv, (x_hi * NZ + b, a * NZ + z),
                ).start()

    def across_copy(b):
        return copy(acc.at[b, core, :, 1 - x_lo], across, across_send, across_recv, neighbour)

    def beside_copy(b, step):
        there = rem(y + step, NY)
        return copy(
            acc.at[b, core, there, x_lo], beside.at[step - 1],
            beside_send, beside_recv, device(x, there, z, core),
        )

    def stage2_across(i):
        b = block(i)
        take_near(b)
        across_copy(b).start()

    def stage3_across(i):
        b = block(i)
        across_copy(b).wait_recv()
        for k in range(NY):
            spot = (b, core, k, x_lo)
            acc[spot] = acc[spot] + across[k]
        for step in (1, 2, 3):
            beside_copy(b, step).start()

    def stage4_across(i):
        b = block(i)
        copy(beside, beside, beside_send, beside_recv, up).wait_recv()
        done[b] = acc[b, core, y, x_lo] + (beside[0] + beside[1] + beside[2])
        go_home(b)

    def prepare():
        all_lists.wait_recv()
        to_scalar = pltpu.make_async_copy(lists, lists_s, local_sem.at[0])
        to_scalar.start()
        for way in (0, 1):
            all_pieces(way)[1].wait_recv()

        @pl.loop(0, CT)
        def _(t):
            place = pl.ds(pl.multiple_of(t * TS, TS), TS)
            for a in range(2):
                value = both[a, :, place]
                high = value.astype(jnp.bfloat16)
                low = (value - high.astype(jnp.float32)).astype(jnp.bfloat16)
                split[t, a * SHARE : (a + 1) * SHARE] = high
                split[t, (2 + a) * SHARE : (3 + a) * SHARE] = low

        to_scalar.wait()

    low = center - core
    early = jnp.logical_or(low < -2, low > NZ)

    def last_near():
        for i in (4, 3, -3):
            near_copy(block(i)).start()

    def last_stage2():
        stage2(4)
        stage2_across(3)
        stage2(-3)

    def tick(t, worked):
        @pl.when(t < PIECES)
        def _():
            for way in (0, 1):
                hop1(way, t).wait_recv()
                hop2(way, t, relayed(way)).start()

        for way in (0, 1):
            arrive(t, way)
        pl.when(t == FIRST)(prepare)
        for stage, i, when in PLAN:
            pl.when(t == when)(lambda: (stage2, stage3, stage4)[stage - 2](i))
        pl.when(both_of(early, t == LAST))(last_near)
        pl.when(both_of(early, t == LAST + 1))(last_stage2)
        stop = jnp.where(t < FIRST, worked, jnp.minimum(worked + MOST, t + 1))
        lax.fori_loop(worked, stop, do_work, 0)
        return stop

    lax.fori_loop(0, TICKS, tick, jnp.int32(-HALF))
    pl.when(jnp.logical_not(early))(last_near)
    stage3(2)
    stage3(-2)
    pl.when(jnp.logical_not(early))(last_stage2)
    stage4(2)
    stage4(-2)
    stage3(4)
    stage3_across(3)
    stage4(4)
    stage3_home(-3)
    stage4_across(3)

    part = landing.at[0, :, pl.ds(0, 4 * TS)]
    copy(part, part, halves_send, out_recv, up).wait_send()
    across_copy(0).wait_send()
    copy(beside, beside, beside_send, beside_recv, up).wait_send()
    all_lists.wait_send()

    for way in (0, 1):
        ring_sent(way)

    for way in (0, 1):
        for made in all_pieces(way):
            made.wait_send()
    copy(near, near, near_send, near_recv.at[0], up).wait_send()
    part = far.at[pl.ds(0, NZ - 1)]
    copy(part, part, far_send, far_recv.at[0], up).wait_send()
    part = pair.at[pl.ds(0, NZ - 2)]
    copy(part, part, pair_send, pair_recv.at[0], up).wait_send()

    way_home = rem(z - rem(col, NZ) + NZ, NZ)
    halved = way_home == NZ - 3
    homes = way_home == 0

    @pl.when(halved)
    def _():
        copy(landing, landing, out_send, out_recv, up).wait_recv()
        out[...] = landing[0] + landing[1]

    @pl.when(homes)
    def _():
        part = landing.at[0, :, pl.ds(0, (RT - 1) * TS)]
        copy(part, part, out_send, out_recv, up).wait_recv()
        part = landing.at[0, :, pl.ds(0, 13 * TS)]
        copy(part, part, out_send, out_recv, up).wait_send()

    @pl.when(jnp.logical_not(homes))
    def _():
        part = landing.at[0, :, pl.ds(0, 14 * TS)]
        copy(part, part, out_send, out_recv, up).wait_send()

    @pl.when(jnp.logical_not(jnp.logical_or(halved, homes)))
    def _():
        copy(landing.at[0], landing.at[0], out_send, out_recv, up).wait_recv()

    @pl.when(jnp.logical_not(halved))
    def _():
        out[...] = landing[0]


def body(tile_values, tile_rows, tile_cols, tile_live, dense_factor):
    dma = pltpu.SemaphoreType.DMA
    vmem = pltpu.VMEM
    f32 = jnp.float32
    return pl.pallas_call(
        kernel,
        out_shape=jax.ShapeDtypeStruct((SHARE, RT * TS), f32),
        in_specs=[pl.BlockSpec(memory_space=pltpu.HBM)] * 5,
        out_specs=pl.BlockSpec(memory_space=pltpu.VMEM),
        scratch_shapes=[
            vmem((NZ, SLOTS, TS, TS), f32),
            vmem((NZ, 3, 1, SLOTS), jnp.int32),
            pltpu.SMEM((NZ, 3, 1, SLOTS), jnp.int32),
            vmem((2, PIECES, SHARE, SPAN), f32),
            vmem((2, SHARE, CT * TS), f32),
            vmem((CT, 4 * SHARE, TS), jnp.bfloat16),
            vmem((NZ, 2, NY, 2, 2 * SHARE, TS), f32),
            vmem((NZ, NY, 2, 2 * SHARE, TS), f32),
            vmem((NZ, 3, 2, 2 * SHARE, TS), f32),
            vmem((NZ, 2 * SHARE, TS), f32),
            vmem((NZ, 2 * SHARE, TS), f32),
            vmem((NY, 2 * SHARE, TS), f32),
            vmem((3, 2 * SHARE, TS), f32),
            vmem((2, SHARE, RT * TS), f32),
            dma((5,)),
            dma, dma((TICKS,)), dma, dma((TICKS,)),
            dma, dma,
            dma((2,)), dma((2, PIECES)), dma((2,)), dma((2,)),
            dma, dma((NZ,)), dma, dma((NZ,)), dma, dma((NZ,)), dma, dma,
            dma, dma, dma, dma, dma,
        ],
        compiler_params=pltpu.CompilerParams(
            collective_id=0, has_side_effects=True, vmem_limit_bytes=56000000
        ),
    )(tile_values[0, 0], tile_rows[0], tile_cols[0], tile_live[0], dense_factor)


def solution(mesh):
    in_specs = (
        P("row", "col", None, None, None),
        P("row", "col", None),
        P("row", "col", None),
        P("row", "col", None),
        P("row", "col"),
    )
    out_specs = P("col", "row")
    return jax.shard_map(body, mesh=mesh, in_specs=in_specs, out_specs=out_specs, check_vma=False)
```

```python
import jax
import jax.numpy as jnp
from jax import lax
from jax.experimental import pallas as pl
from jax.experimental.pallas import tpu as pltpu
from jax.sharding import PartitionSpec as P

NX, NY, NZ = 4, 4, 8
TS = 128
SHARE = 32
RT = 16
CT = 64
SLOTS = 16
PER = 2
CHUNKS = SLOTS // PER
HALF = CHUNKS // 2
PIECES = 4
SPAN = CT * TS // (2 * PIECES)
GROUPS = 5
TICKS = GROUPS * HALF
NONE = 2 * GROUPS
LAST = 17
FIRST = 7
MOST = 4
PLAN = (
    (2, 0, 9), (2, 1, 10), (2, -1, 11), (3, 0, 12), (3, 1, 13), (3, -1, 14),
    (4, 0, 15), (4, 1, 16), (2, 2, 16), (2, -2, 17), (4, -1, 17),
)
MESH = pl.DeviceIdType.MESH


def rem(a, b):
    return lax.rem(a, jnp.int32(b))


def div(a, b):
    return lax.div(a, jnp.int32(b))


def kernel(
    tiles, rows_in, cols_in, live_in, dense, out,
    held, lists, lists_s, relay, both, split, acc, near, far, pair, done, across, beside, landing,
    local_sem,
    right_send, right_recv, left_send, left_recv, list_send, list_recv,
    hop1_send, hop1_recv, hop2_send, hop2_recv,
    near_send, near_recv, far_send, far_recv, pair_send, pair_recv, out_send, out_recv,
    across_send, across_recv, beside_send, beside_recv, halves_send,
):
    row, col = lax.axis_index("row"), lax.axis_index("col")
    x_hi, z = div(row, NZ), rem(row, NZ)
    y, x_lo, core = div(col, 4), rem(div(col, 2), 2), rem(col, 2)
    x = x_hi * 2 + x_lo

    def device(x, y, z, core):
        return (div(x, 2) * NZ + z, y * 4 + rem(x, 2) * 2 + core)

    def copy(src, dst, send_sem, recv_sem, target):
        return pltpu.make_async_remote_copy(
            src_ref=src, dst_ref=dst, send_sem=send_sem, recv_sem=recv_sem,
            device_id=target, device_id_type=MESH,
        )

    up = device(x, y, rem(z + 1, NZ), core)
    down = device(x, y, rem(z + NZ - 1, NZ), core)
    forth = device(rem(x + 1, NX), y, z, core)
    back = device(rem(x + NX - 1, NX), y, z, core)

    barrier = pltpu.get_barrier_semaphore()
    partners = [device(x, y, rem(z + step, NZ), core) for step in range(1, NZ)]
    partners += [forth, back, device(x, y, z, 1 - core)]
    partners += [device(x, rem(y + step, NY), z, core) for step in (1, 2, 3)]
    for partner in partners:
        pl.semaphore_signal(barrier, inc=1, device_id=partner, device_id_type=MESH)

    center = col - x_hi * NZ

    def banded(source):
        gap = source - center
        return jnp.logical_and(gap >= -1, gap <= 1)

    both_of = jnp.logical_and
    crossed = jnp.logical_and(center >= -1, center <= NZ)

    def place(source):
        return rem(source - center + 3 + 4 * NZ, NZ) - 3

    def hops(source, half, way):
        u = place(source)
        first = jnp.where(u > 0, 4, 3)
        second = jnp.where(u < 0, 2, jnp.where(u > 0, 5, 4))
        even = 3 + rem(source, 2)
        rightwards = jnp.where(crossed, jnp.where(half == 1, second, first), even)
        return rightwards if way == 0 else NZ - 1 - rightwards

    def half_of(source, turn, way):
        swap = (place(source) >= 0) if way == 0 else (place(source) < 0)
        return rem(turn + jnp.where(swap, 1, 0), 2)

    def travels(source, half, level, way):
        there = jnp.logical_or(half == 0, banded(source))
        return jnp.logical_and(there, level < hops(source, half, way))

    def source_of(level, way):
        return rem(z + 2 * NZ + (-level - 1 if way == 0 else level + 1), NZ)

    own_groups = jnp.where(banded(z), 2, 1)
    coming, passed, onward = [], [], []
    for way in (0, 1):
        group = [jnp.int32(NONE)] * GROUPS
        count = jnp.int32(0)
        for g in range(2 * GROUPS):
            source = source_of(g // 2, way)
            there = travels(source, half_of(source, g % 2, way), g // 2, way)
            for n in range(GROUPS):
                group[n] = jnp.where(jnp.logical_and(there, count == n), g, group[n])
            count = count + jnp.where(there, 1, 0)
        coming.append(group)
        goes, slots = [], []
        slot = own_groups
        for n in range(GROUPS):
            level = div(group[n], 2)
            source = source_of(level, way)
            on = travels(source, half_of(source, rem(group[n], 2), way), level + 1, way)
            on = jnp.logical_and(on, group[n] < NONE)
            goes.append(jnp.where(on, 1, 0))
            slots.append(slot)
            slot = slot + goes[-1]
        passed.append(goes)
        onward.append(slots)

    def pick(values, n):
        chosen = values[0]
        for i in range(1, GROUPS):
            chosen = jnp.where(n == i, values[i], chosen)
        return chosen

    def ring_copy(source, j, slot, way):
        part = held.at[source, pl.ds(PER * j, PER)]
        if way == 0:
            return copy(part, part, right_send, right_recv.at[slot], up)
        return copy(part, part, left_send, left_recv.at[slot], down)

    def message(t, way):
        group = pick(coming[way], div(t, HALF))
        source = source_of(div(group, 2), way)
        j = half_of(source, rem(group, 2), way) * HALF + rem(t, HALF)
        return group < NONE, source, j

    def arrive(t, way):
        there, source, j = message(t, way)

        @pl.when(there)
        def _():
            ring_copy(source, j, t, way).wait_recv()
            n = div(t, HALF)

            @pl.when(pick(passed[way], n) == 1)
            def _():
                ring_copy(source, j, pick(onward[way], n) * HALF + rem(t, HALF), way).start()

    def own_message(k, way):
        turn = div(k, HALF)
        half = jnp.where(own_groups == 2, half_of(z, turn, way), 0)
        return turn < own_groups, ring_copy(z, half * HALF + rem(k, HALF), k, way)

    def ring_sent(way):
        count = own_groups
        for n in range(GROUPS):
            count = count + passed[way][n]
        for c in range(1, GROUPS + 1):
            part = held.at[pl.ds(0, c), pl.ds(0, PER * HALF)]
            sem = right_send if way == 0 else left_send
            pl.when(count == c)(copy(part, part, sem, right_recv.at[0], up).wait_send)

    def list_copy(p):
        peer = rem(z + p, NZ)
        return copy(lists.at[z], lists.at[z], list_send, list_recv, device(x, y, peer, core))

    seven = lists.at[pl.ds(0, NZ - 1)]
    all_lists = copy(seven, seven, list_send, list_recv, up)

    def columns(way, k):
        return pl.ds(pl.multiple_of((way * PIECES + k) * SPAN, SPAN), SPAN)

    def hop1(way, k):
        return copy(
            both.at[x_hi, :, columns(way, k)], relay.at[way, k],
            hop1_send.at[way], hop1_recv.at[way, k], (forth, back)[way],
        )

    def hop2(way, k, owner):
        return copy(
            relay.at[way, k], both.at[owner, :, columns(way, k)],
            hop2_send.at[way], hop2_recv.at[way], (forth, back)[way],
        )

    def all_pieces(way):
        part = both.at[1 - x_hi, :, pl.ds(way * PIECES * SPAN, PIECES * SPAN)]
        return (
            copy(part, part, hop1_send.at[way], hop2_recv.at[way], forth),
            copy(part, part, hop2_send.at[way], hop2_recv.at[way], forth),
        )

    def relayed(way):
        return div(rem(x + (NX - 1 if way == 0 else 1), NX), 2)

    own_lists = [
        pltpu.make_async_copy(ref, lists.at[z, k], local_sem.at[k])
        for k, ref in enumerate((rows_in, cols_in, live_in))
    ]

    own_tiles = pltpu.make_async_copy(tiles, held.at[z], local_sem.at[3])
    own_dense = pltpu.make_async_copy(dense, both.at[x_hi], local_sem.at[4])
    for made in own_lists:
        made.start()
    own_tiles.start()
    own_dense.start()

    for made in own_lists:
        made.wait()
    own_tiles.wait()
    pl.semaphore_wait(barrier, len(partners))

    @pl.loop(1, NZ)
    def _(p):
        list_copy(p).start()

    @pl.loop(0, CHUNKS)
    def _(k):
        for way in (0, 1):
            there, made = own_message(k, way)
            pl.when(there)(made.start)

    own_dense.wait()

    @pl.loop(0, PIECES)
    def _(k):
        for way in (0, 1):
            hop1(way, k).start()

    @pl.loop(0, NZ * RT)
    def _(i):
        acc[div(i, RT), div(rem(i, RT), 8), div(rem(i, 8), 2), rem(i, 2)] = jnp.zeros(
            (2 * SHARE, TS), jnp.float32
        )

    def one_tile(b, slot):
        tile = held[b, slot]
        high = tile.astype(jnp.bfloat16)
        low = (tile - high.astype(jnp.float32)).astype(jnp.bfloat16)
        chosen = split[lists_s[b, 1, 0, slot]]
        dims = (((1,), (1,)), ((), ()))
        by_high = lax.dot_general(chosen, high, dims, preferred_element_type=jnp.float32)
        by_low = lax.dot_general(
            chosen[: 2 * SHARE], low, dims, preferred_element_type=jnp.float32
        )
        return by_high[: 2 * SHARE] + (by_high[2 * SHARE :] + by_low)

    def multiply(*messages):
        products = [[one_tile(b, PER * j + s) for s in range(PER)] for b, j in messages]
        for (b, j), pair_of in zip(messages, products):
            slots = [PER * j + s for s in range(PER)]
            lives = [lists_s[b, 2, 0, slot].astype(jnp.float32) for slot in slots]
            for k in range(RT):
                place_of = (b, k // 8, k // 2 % NY, k % 2)
                term = acc[place_of]
                for s in range(PER):
                    weight = jnp.where(lists_s[b, 0, 0, slots[s]] == k, lives[s], 0.0)
                    term = term + weight * pair_of[s]
                acc[place_of] = term

    def do_work(w, carry):
        @pl.when(both_of(w < 0, 2 * (w + HALF) < own_groups * HALF))
        def _():
            multiply((z, 2 * (w + HALF)), (z, 2 * (w + HALF) + 1))

        @pl.when(w >= 0)
        def _():
            there, source, j = message(w, 0)
            there_too, source_too, j_too = message(w, 1)
            pl.when(both_of(there, there_too))(lambda: multiply((source, j), (source_too, j_too)))
            alone, alone_j = jnp.where(there, source, source_too), jnp.where(there, j, j_too)
            pl.when(there != there_too)(lambda: multiply((alone, alone_j)))

        for i, when in ((0, -1), (1, 2 * HALF - 1), (-1, 2 * HALF - 1), (2, 4 * HALF - 1), (-2, 4 * HALF - 1)):
            pl.when(w == when)(lambda: near_copy(block(i)).start())
        return carry

    def block(i):
        return rem(z + i + NZ, NZ)

    def near_copy(b):
        return copy(
            acc.at[b, 1 - core], near.at[b],
            near_send, near_recv.at[b], device(x, y, z, 1 - core),
        )

    def far_copy(b, step):
        there = rem(y + step, NY)
        return copy(
            acc.at[b, core, there], far.at[b, step - 1],
            far_send, far_recv.at[b], device(x, there, z, core),
        )

    neighbour = device(x_hi * 2 + 1 - x_lo, y, z, core)

    def pair_copy(b):
        return copy(acc.at[b, core, y, 1 - x_lo], pair.at[b], pair_send, pair_recv.at[b], neighbour)

    def tile_row(k):
        return pl.ds(pl.multiple_of((core * 8 + y * 2 + k) * TS, TS), TS)

    def out_copy(b, a):
        return copy(
            done.at[b, pl.ds(a * SHARE, SHARE)], landing.at[0, :, tile_row(x_lo)],
            out_send, out_recv, (x_hi * NZ + b, a * NZ + z),
        )

    def is_home(b, a):
        return jnp.logical_and(b == z, a * NZ + z == col)

    def go_home(b):
        for a in range(2):
            home = is_home(b, a)

            @pl.when(home)
            def _():
                landing[0, :, tile_row(x_lo)] = done[b, a * SHARE : (a + 1) * SHARE]

            pl.when(jnp.logical_not(home))(out_copy(b, a).start)

    def take_near(b):
        near_copy(b).wait_recv()

        @pl.loop(0, 8)
        def _(k):
            spot = (b, core, div(k, 2), rem(k, 2))
            acc[spot] = acc[spot] + near[b, div(k, 2), rem(k, 2)]

    def take_far(b):
        copy(far.at[b], far.at[b], far_send, far_recv.at[b], up).wait_recv()
        for k in range(2):
            spot = (b, core, y, k)
            acc[spot] = acc[spot] + (far[b, 0, k] + far[b, 1, k] + far[b, 2, k])

    def stage2(i):
        b = block(i)
        take_near(b)
        for step in (1, 2, 3):
            far_copy(b, step).start()

    def stage3(i):
        b = block(i)
        take_far(b)
        pair_copy(b).start()

    def stage4(i):
        b = block(i)
        pair_copy(b).wait_recv()
        done[b] = acc[b, core, y, x_lo] + pair[b]
        go_home(b)

    def stage3_home(i):
        b = block(i)
        take_far(b)
        for k in range(2):
            for a in range(2):
                copy(
                    acc.at[b, core, y, k, pl.ds(a * SHARE, SHARE)], landing.at[x_lo, :, tile_row(k)],
                    halves_send, out_recv, (x_hi * NZ + b, a * NZ + z),
                ).start()

    def across_copy(b):
        return copy(acc.at[b, core, :, 1 - x_lo], across, across_send, across_recv, neighbour)

    def beside_copy(b, step):
        there = rem(y + step, NY)
        return copy(
            acc.at[b, core, there, x_lo], beside.at[step - 1],
            beside_send, beside_recv, device(x, there, z, core),
        )

    def stage2_across(i):
        b = block(i)
        take_near(b)
        across_copy(b).start()

    def stage3_across(i):
        b = block(i)
        across_copy(b).wait_recv()
        for k in range(NY):
            spot = (b, core, k, x_lo)
            acc[spot] = acc[spot] + across[k]
        for step in (1, 2, 3):
            beside_copy(b, step).start()

    def stage4_across(i):
        b = block(i)
        copy(beside, beside, beside_send, beside_recv, up).wait_recv()
        done[b] = acc[b, core, y, x_lo] + (beside[0] + beside[1] + beside[2])
        go_home(b)

    def prepare():
        all_lists.wait_recv()
        to_scalar = pltpu.make_async_copy(lists, lists_s, local_sem.at[0])
        to_scalar.start()
        for way in (0, 1):
            all_pieces(way)[1].wait_recv()

        @pl.loop(0, CT)
        def _(t):
            place = pl.ds(pl.multiple_of(t * TS, TS), TS)
            for a in range(2):
                value = both[a, :, place]
                high = value.astype(jnp.bfloat16)
                low = (value - high.astype(jnp.float32)).astype(jnp.bfloat16)
                split[t, a * SHARE : (a + 1) * SHARE] = high
                split[t, (2 + a) * SHARE : (3 + a) * SHARE] = low

        to_scalar.wait()

    low = center - core
    early = jnp.logical_or(low < -2, low > NZ)

    def last_near():
        for i in (4, 3, -3):
            near_copy(block(i)).start()

    def last_stage2():
        stage2(4)
        stage2_across(3)
        stage2(-3)

    def tick(t, worked):
        @pl.when(t < PIECES)
        def _():
            for way in (0, 1):
                hop1(way, t).wait_recv()
                hop2(way, t, relayed(way)).start()

        for way in (0, 1):
            arrive(t, way)
        pl.when(t == FIRST)(prepare)
        for stage, i, when in PLAN:
            pl.when(t == when)(lambda: (stage2, stage3, stage4)[stage - 2](i))
        pl.when(both_of(early, t == LAST))(last_near)
        pl.when(both_of(early, t == LAST + 1))(last_stage2)
        stop = jnp.where(t < FIRST, worked, jnp.minimum(worked + MOST, t + 1))
        lax.fori_loop(worked, stop, do_work, 0)
        return stop

    lax.fori_loop(0, TICKS, tick, jnp.int32(-HALF))
    pl.when(jnp.logical_not(early))(last_near)
    stage3(2)
    stage3(-2)
    pl.when(jnp.logical_not(early))(last_stage2)
    stage4(2)
    stage4(-2)
    stage3(4)
    stage3_across(3)
    stage4(4)
    stage3_home(-3)
    stage4_across(3)

    part = landing.at[0, :, pl.ds(0, 4 * TS)]
    copy(part, part, halves_send, out_recv, up).wait_send()
    across_copy(0).wait_send()
    copy(beside, beside, beside_send, beside_recv, up).wait_send()
    all_lists.wait_send()

    for way in (0, 1):
        ring_sent(way)

    for way in (0, 1):
        for made in all_pieces(way):
            made.wait_send()
    copy(near, near, near_send, near_recv.at[0], up).wait_send()
    part = far.at[pl.ds(0, NZ - 1)]
    copy(part, part, far_send, far_recv.at[0], up).wait_send()
    part = pair.at[pl.ds(0, NZ - 2)]
    copy(part, part, pair_send, pair_recv.at[0], up).wait_send()

    way_home = rem(z - rem(col, NZ) + NZ, NZ)
    halved = way_home == NZ - 3
    homes = way_home == 0

    @pl.when(halved)
    def _():
        copy(landing, landing, out_send, out_recv, up).wait_recv()
        out[...] = landing[0] + landing[1]

    @pl.when(homes)
    def _():
        part = landing.at[0, :, pl.ds(0, (RT - 1) * TS)]
        copy(part, part, out_send, out_recv, up).wait_recv()
        part = landing.at[0, :, pl.ds(0, 13 * TS)]
        copy(part, part, out_send, out_recv, up).wait_send()

    @pl.when(jnp.logical_not(homes))
    def _():
        part = landing.at[0, :, pl.ds(0, 14 * TS)]
        copy(part, part, out_send, out_recv, up).wait_send()

    @pl.when(jnp.logical_not(jnp.logical_or(halved, homes)))
    def _():
        copy(landing.at[0], landing.at[0], out_send, out_recv, up).wait_recv()

    @pl.when(jnp.logical_not(halved))
    def _():
        out[...] = landing[0]


def body(tile_values, tile_rows, tile_cols, tile_live, dense_factor):
    dma = pltpu.SemaphoreType.DMA
    vmem = pltpu.VMEM
    f32 = jnp.float32
    return pl.pallas_call(
        kernel,
        out_shape=jax.ShapeDtypeStruct((SHARE, RT * TS), f32),
        in_specs=[pl.BlockSpec(memory_space=pltpu.HBM)] * 5,
        out_specs=pl.BlockSpec(memory_space=pltpu.VMEM),
        scratch_shapes=[
            vmem((NZ, SLOTS, TS, TS), f32),
            vmem((NZ, 3, 1, SLOTS), jnp.int32),
            pltpu.SMEM((NZ, 3, 1, SLOTS), jnp.int32),
            vmem((2, PIECES, SHARE, SPAN), f32),
            vmem((2, SHARE, CT * TS), f32),
            vmem((CT, 4 * SHARE, TS), jnp.bfloat16),
            vmem((NZ, 2, NY, 2, 2 * SHARE, TS), f32),
            vmem((NZ, NY, 2, 2 * SHARE, TS), f32),
            vmem((NZ, 3, 2, 2 * SHARE, TS), f32),
            vmem((NZ, 2 * SHARE, TS), f32),
            vmem((NZ, 2 * SHARE, TS), f32),
            vmem((NY, 2 * SHARE, TS), f32),
            vmem((3, 2 * SHARE, TS), f32),
            vmem((2, SHARE, RT * TS), f32),
            dma((5,)),
            dma, dma((TICKS,)), dma, dma((TICKS,)),
            dma, dma,
            dma((2,)), dma((2, PIECES)), dma((2,)), dma((2,)),
            dma, dma((NZ,)), dma, dma((NZ,)), dma, dma((NZ,)), dma, dma,
            dma, dma, dma, dma, dma,
        ],
        compiler_params=pltpu.CompilerParams(
            collective_id=0, has_side_effects=True, vmem_limit_bytes=56000000
        ),
    )(
        *(
            pltpu.with_memory_space_constraint(value, pltpu.HBM)
            for value in (tile_values[0, 0], tile_rows[0], tile_cols[0], tile_live[0], dense_factor)
        )
    )


def solution(mesh):
    in_specs = (
        P("row", "col", None, None, None),
        P("row", "col", None),
        P("row", "col", None),
        P("row", "col", None),
        P("row", "col"),
    )
    out_specs = P("col", "row")
    return jax.shard_map(body, mesh=mesh, in_specs=in_specs, out_specs=out_specs, check_vma=False)
```

```python
import jax
import jax.numpy as jnp
from jax import lax
from jax.experimental import pallas as pl
from jax.experimental.pallas import tpu as pltpu
from jax.sharding import PartitionSpec as P

NX, NY, NZ = 4, 4, 8
TS = 128
SHARE = 32
RT = 16
CT = 64
SLOTS = 16
PER = 2
CHUNKS = SLOTS // PER
HALF = CHUNKS // 2
PIECES = 4
SPAN = CT * TS // (2 * PIECES)
GROUPS = 5
TICKS = GROUPS * HALF
NONE = 2 * GROUPS
LAST = 17
EARLY = 4
FIRST = 7
MOST = 4
PLAN = (
    (2, 0, 9), (2, 1, 10), (2, -1, 11), (3, 0, 12), (3, 1, 13), (3, -1, 14),
    (4, 0, 15), (4, 1, 16), (2, 2, 16), (2, -2, 17), (4, -1, 17),
)
MESH = pl.DeviceIdType.MESH


def rem(a, b):
    return lax.rem(a, jnp.int32(b))


def div(a, b):
    return lax.div(a, jnp.int32(b))


def kernel(
    tiles, rows_in, cols_in, live_in, dense, out,
    held, lists, lists_s, relay, both, split, acc, near, far, pair, done, across, beside, landing,
    word, local_sem,
    right_send, right_recv, left_send, left_recv, list_send, list_recv,
    hop1_send, hop1_recv, hop2_send, hop2_recv,
    near_send, near_recv, far_send, far_recv, pair_send, pair_recv, out_send, out_recv,
    across_send, across_recv, beside_send, beside_recv, halves_send,
):
    row, col = lax.axis_index("row"), lax.axis_index("col")
    x_hi, z = div(row, NZ), rem(row, NZ)
    y, x_lo, core = div(col, 4), rem(div(col, 2), 2), rem(col, 2)
    x = x_hi * 2 + x_lo

    def device(x, y, z, core):
        return (div(x, 2) * NZ + z, y * 4 + rem(x, 2) * 2 + core)

    def copy(src, dst, send_sem, recv_sem, target):
        return pltpu.make_async_remote_copy(
            src_ref=src, dst_ref=dst, send_sem=send_sem, recv_sem=recv_sem,
            device_id=target, device_id_type=MESH,
        )

    up = device(x, y, rem(z + 1, NZ), core)
    down = device(x, y, rem(z + NZ - 1, NZ), core)
    forth = device(rem(x + 1, NX), y, z, core)
    back = device(rem(x + NX - 1, NX), y, z, core)

    barrier = pltpu.get_barrier_semaphore()
    partners = [up, down, forth, back, device(x, y, z, 1 - core)]
    partners += [device(x, rem(y + step, NY), z, core) for step in (1, 2, 3)]
    for partner in partners:
        pl.semaphore_signal(barrier, inc=1, device_id=partner, device_id_type=MESH)

    center = col - x_hi * NZ

    def banded(source):
        gap = source - center
        return jnp.logical_and(gap >= -1, gap <= 1)

    both_of = jnp.logical_and
    crossed = jnp.logical_and(center >= -1, center <= NZ)

    def place(source):
        return rem(source - center + 3 + 4 * NZ, NZ) - 3

    def hops(source, half, way):
        u = place(source)
        first = jnp.where(u > 0, 4, 3)
        second = jnp.where(u < 0, 2, jnp.where(u > 0, 5, 4))
        even = 3 + rem(source, 2)
        rightwards = jnp.where(crossed, jnp.where(half == 1, second, first), even)
        return rightwards if way == 0 else NZ - 1 - rightwards

    def half_of(source, turn, way):
        swap = (place(source) >= 0) if way == 0 else (place(source) < 0)
        return rem(turn + jnp.where(swap, 1, 0), 2)

    def travels(source, half, level, way):
        there = jnp.logical_or(half == 0, banded(source))
        return jnp.logical_and(there, level < hops(source, half, way))

    def source_of(level, way):
        return rem(z + 2 * NZ + (-level - 1 if way == 0 else level + 1), NZ)

    own_groups = jnp.where(banded(z), 2, 1)
    coming, passed, onward = [], [], []
    for way in (0, 1):
        group = [jnp.int32(NONE)] * GROUPS
        count = jnp.int32(0)
        for g in range(2 * GROUPS):
            source = source_of(g // 2, way)
            there = travels(source, half_of(source, g % 2, way), g // 2, way)
            for n in range(GROUPS):
                group[n] = jnp.where(jnp.logical_and(there, count == n), g, group[n])
            count = count + jnp.where(there, 1, 0)
        coming.append(group)
        goes, slots = [], []
        slot = own_groups
        for n in range(GROUPS):
            level = div(group[n], 2)
            source = source_of(level, way)
            on = travels(source, half_of(source, rem(group[n], 2), way), level + 1, way)
            on = jnp.logical_and(on, group[n] < NONE)
            goes.append(jnp.where(on, 1, 0))
            slots.append(slot)
            slot = slot + goes[-1]
        passed.append(goes)
        onward.append(slots)

    def pick(values, n):
        chosen = values[0]
        for i in range(1, GROUPS):
            chosen = jnp.where(n == i, values[i], chosen)
        return chosen

    def ring_copy(source, j, slot, way):
        part = held.at[source, pl.ds(PER * j, PER)]
        if way == 0:
            return copy(part, part, right_send, right_recv.at[slot], up)
        return copy(part, part, left_send, left_recv.at[slot], down)

    def message(t, way):
        group = pick(coming[way], div(t, HALF))
        source = source_of(div(group, 2), way)
        j = half_of(source, rem(group, 2), way) * HALF + rem(t, HALF)
        return group < NONE, source, j

    def arrive(t, way):
        there, source, j = message(t, way)

        @pl.when(there)
        def _():
            ring_copy(source, j, t, way).wait_recv()
            n = div(t, HALF)

            @pl.when(pick(passed[way], n) == 1)
            def _():
                ring_copy(source, j, pick(onward[way], n) * HALF + rem(t, HALF), way).start()

    def own_message(k, way):
        turn = div(k, HALF)
        half = jnp.where(own_groups == 2, half_of(z, turn, way), 0)
        return turn < own_groups, ring_copy(z, half * HALF + rem(k, HALF), k, way)

    def ring_sent(way):
        count = own_groups
        for n in range(GROUPS):
            count = count + passed[way][n]
        for c in range(1, GROUPS + 1):
            part = held.at[pl.ds(0, c), pl.ds(0, PER * HALF)]
            sem = right_send if way == 0 else left_send
            pl.when(count == c)(copy(part, part, sem, right_recv.at[0], up).wait_send)

    def list_copy(p):
        peer = rem(z + p, NZ)
        return copy(lists.at[z], lists.at[z], list_send, list_recv, device(x, y, peer, core))

    seven = lists.at[pl.ds(0, NZ - 1)]
    all_lists = copy(seven, seven, list_send, list_recv, up)

    def columns(way, k):
        return pl.ds(pl.multiple_of((way * PIECES + k) * SPAN, SPAN), SPAN)

    def hop1(way, k):
        return copy(
            both.at[x_hi, :, columns(way, k)], relay.at[way, k],
            hop1_send.at[way], hop1_recv.at[way, k], (forth, back)[way],
        )

    def hop2(way, k, owner):
        return copy(
            relay.at[way, k], both.at[owner, :, columns(way, k)],
            hop2_send.at[way], hop2_recv.at[way], (forth, back)[way],
        )

    def all_pieces(way):
        part = both.at[1 - x_hi, :, pl.ds(way * PIECES * SPAN, PIECES * SPAN)]
        return (
            copy(part, part, hop1_send.at[way], hop2_recv.at[way], forth),
            copy(part, part, hop2_send.at[way], hop2_recv.at[way], forth),
        )

    def relayed(way):
        return div(rem(x + (NX - 1 if way == 0 else 1), NX), 2)

    own_lists = [
        pltpu.make_async_copy(ref, lists.at[z, k], local_sem.at[k])
        for k, ref in enumerate((rows_in, cols_in, live_in))
    ]

    own_tiles = pltpu.make_async_copy(tiles, held.at[z], local_sem.at[3])
    own_dense = pltpu.make_async_copy(dense, both.at[x_hi], local_sem.at[4])
    for made in own_lists:
        made.start()
    own_tiles.start()
    own_dense.start()

    for made in own_lists:
        made.wait()
    own_tiles.wait()
    pl.semaphore_wait(barrier, len(partners))

    def own_start(k):
        for way in (0, 1):
            there, made = own_message(k, way)
            pl.when(there)(made.start)

    for k in range(EARLY):
        own_start(k)
    own_dense.wait()

    @pl.loop(0, PIECES)
    def _(k):
        for way in (0, 1):
            hop1(way, k).start()

    for step in range(NZ // 2 - 1):
        for side, target in enumerate((up, down)):
            pl.semaphore_signal(word.at[step, side], inc=1, device_id=target, device_id_type=MESH)
        for side in (0, 1):
            pl.semaphore_wait(word.at[step, side], 1)

    @pl.loop(1, NZ)
    def _(p):
        list_copy(p).start()

    @pl.loop(EARLY, CHUNKS)
    def _(k):
        own_start(k)

    @pl.loop(0, NZ * RT)
    def _(i):
        acc[div(i, RT), div(rem(i, RT), 8), div(rem(i, 8), 2), rem(i, 2)] = jnp.zeros(
            (2 * SHARE, TS), jnp.float32
        )

    def one_tile(b, slot):
        tile = held[b, slot]
        high = tile.astype(jnp.bfloat16)
        low = (tile - high.astype(jnp.float32)).astype(jnp.bfloat16)
        chosen = split[lists_s[b, 1, 0, slot]]
        dims = (((1,), (1,)), ((), ()))
        by_high = lax.dot_general(chosen, high, dims, preferred_element_type=jnp.float32)
        by_low = lax.dot_general(
            chosen[: 2 * SHARE], low, dims, preferred_element_type=jnp.float32
        )
        return by_high[: 2 * SHARE] + (by_high[2 * SHARE :] + by_low)

    def multiply(*messages):
        products = [[one_tile(b, PER * j + s) for s in range(PER)] for b, j in messages]
        for (b, j), pair_of in zip(messages, products):
            slots = [PER * j + s for s in range(PER)]
            lives = [lists_s[b, 2, 0, slot].astype(jnp.float32) for slot in slots]
            for k in range(RT):
                place_of = (b, k // 8, k // 2 % NY, k % 2)
                term = acc[place_of]
                for s in range(PER):
                    weight = jnp.where(lists_s[b, 0, 0, slots[s]] == k, lives[s], 0.0)
                    term = term + weight * pair_of[s]
                acc[place_of] = term

    def do_work(w, carry):
        @pl.when(both_of(w < 0, 2 * (w + HALF) < own_groups * HALF))
        def _():
            multiply((z, 2 * (w + HALF)), (z, 2 * (w + HALF) + 1))

        @pl.when(w >= 0)
        def _():
            there, source, j = message(w, 0)
            there_too, source_too, j_too = message(w, 1)
            pl.when(both_of(there, there_too))(lambda: multiply((source, j), (source_too, j_too)))
            alone, alone_j = jnp.where(there, source, source_too), jnp.where(there, j, j_too)
            pl.when(there != there_too)(lambda: multiply((alone, alone_j)))

        for i, when in ((0, -1), (1, 2 * HALF - 1), (-1, 2 * HALF - 1), (2, 4 * HALF - 1), (-2, 4 * HALF - 1)):
            pl.when(w == when)(lambda: near_copy(block(i)).start())
        return carry

    def block(i):
        return rem(z + i + NZ, NZ)

    def near_copy(b):
        return copy(
            acc.at[b, 1 - core], near.at[b],
            near_send, near_recv.at[b], device(x, y, z, 1 - core),
        )

    def far_copy(b, step):
        there = rem(y + step, NY)
        return copy(
            acc.at[b, core, there], far.at[b, step - 1],
            far_send, far_recv.at[b], device(x, there, z, core),
        )

    neighbour = device(x_hi * 2 + 1 - x_lo, y, z, core)

    def pair_copy(b):
        return copy(acc.at[b, core, y, 1 - x_lo], pair.at[b], pair_send, pair_recv.at[b], neighbour)

    def tile_row(k):
        return pl.ds(pl.multiple_of((core * 8 + y * 2 + k) * TS, TS), TS)

    def out_copy(b, a):
        return copy(
            done.at[b, pl.ds(a * SHARE, SHARE)], landing.at[0, :, tile_row(x_lo)],
            out_send, out_recv, (x_hi * NZ + b, a * NZ + z),
        )

    def is_home(b, a):
        return jnp.logical_and(b == z, a * NZ + z == col)

    def go_home(b):
        for a in range(2):
            home = is_home(b, a)

            @pl.when(home)
            def _():
                landing[0, :, tile_row(x_lo)] = done[b, a * SHARE : (a + 1) * SHARE]

            pl.when(jnp.logical_not(home))(out_copy(b, a).start)

    def take_near(b):
        near_copy(b).wait_recv()

        @pl.loop(0, 8)
        def _(k):
            spot = (b, core, div(k, 2), rem(k, 2))
            acc[spot] = acc[spot] + near[b, div(k, 2), rem(k, 2)]

    def take_far(b):
        copy(far.at[b], far.at[b], far_send, far_recv.at[b], up).wait_recv()
        for k in range(2):
            spot = (b, core, y, k)
            acc[spot] = acc[spot] + (far[b, 0, k] + far[b, 1, k] + far[b, 2, k])

    def stage2(i):
        b = block(i)
        take_near(b)
        for step in (1, 2, 3):
            far_copy(b, step).start()

    def stage3(i):
        b = block(i)
        take_far(b)
        pair_copy(b).start()

    def stage4(i):
        b = block(i)
        pair_copy(b).wait_recv()
        done[b] = acc[b, core, y, x_lo] + pair[b]
        go_home(b)

    def stage3_home(i):
        b = block(i)
        take_far(b)
        for k in range(2):
            for a in range(2):
                copy(
                    acc.at[b, core, y, k, pl.ds(a * SHARE, SHARE)], landing.at[x_lo, :, tile_row(k)],
                    halves_send, out_recv, (x_hi * NZ + b, a * NZ + z),
                ).start()

    def across_copy(b):
        return copy(acc.at[b, core, :, 1 - x_lo], across, across_send, across_recv, neighbour)

    def beside_copy(b, step):
        there = rem(y + step, NY)
        return copy(
            acc.at[b, core, there, x_lo], beside.at[step - 1],
            beside_send, beside_recv, device(x, there, z, core),
        )

    def stage2_across(i):
        b = block(i)
        take_near(b)
        across_copy(b).start()

    def stage3_across(i):
        b = block(i)
        across_copy(b).wait_recv()
        for k in range(NY):
            spot = (b, core, k, x_lo)
            acc[spot] = acc[spot] + across[k]
        for step in (1, 2, 3):
            beside_copy(b, step).start()

    def stage4_across(i):
        b = block(i)
        copy(beside, beside, beside_send, beside_recv, up).wait_recv()
        done[b] = acc[b, core, y, x_lo] + (beside[0] + beside[1] + beside[2])
        go_home(b)

    def prepare():
        all_lists.wait_recv()
        to_scalar = pltpu.make_async_copy(lists, lists_s, local_sem.at[0])
        to_scalar.start()
        for way in (0, 1):
            all_pieces(way)[1].wait_recv()

        @pl.loop(0, CT)
        def _(t):
            place = pl.ds(pl.multiple_of(t * TS, TS), TS)
            for a in range(2):
                value = both[a, :, place]
                high = value.astype(jnp.bfloat16)
                low = (value - high.astype(jnp.float32)).astype(jnp.bfloat16)
                split[t, a * SHARE : (a + 1) * SHARE] = high
                split[t, (2 + a) * SHARE : (3 + a) * SHARE] = low

        to_scalar.wait()

    low = center - core
    early = jnp.logical_or(low < -2, low > NZ)

    def last_near():
        for i in (4, 3, -3):
            near_copy(block(i)).start()

    def last_stage2():
        stage2(4)
        stage2_across(3)
        stage2(-3)

    def tick(t, worked):
        @pl.when(t < PIECES)
        def _():
            for way in (0, 1):
                hop1(way, t).wait_recv()
                hop2(way, t, relayed(way)).start()

        for way in (0, 1):
            arrive(t, way)
        pl.when(t == FIRST)(prepare)
        for stage, i, when in PLAN:
            pl.when(t == when)(lambda: (stage2, stage3, stage4)[stage - 2](i))
        pl.when(both_of(early, t == LAST))(last_near)
        pl.when(both_of(early, t == LAST + 1))(last_stage2)
        stop = jnp.where(t < FIRST, worked, jnp.minimum(worked + MOST, t + 1))
        lax.fori_loop(worked, stop, do_work, 0)
        return stop

    lax.fori_loop(0, TICKS, tick, jnp.int32(-HALF))
    pl.when(jnp.logical_not(early))(last_near)
    stage3(2)
    stage3(-2)
    pl.when(jnp.logical_not(early))(last_stage2)
    stage4(2)
    stage4(-2)
    stage3(4)
    stage3_across(3)
    stage4(4)
    stage3_home(-3)
    stage4_across(3)

    part = landing.at[0, :, pl.ds(0, 4 * TS)]
    copy(part, part, halves_send, out_recv, up).wait_send()
    across_copy(0).wait_send()
    copy(beside, beside, beside_send, beside_recv, up).wait_send()
    all_lists.wait_send()

    for way in (0, 1):
        ring_sent(way)

    for way in (0, 1):
        for made in all_pieces(way):
            made.wait_send()
    copy(near, near, near_send, near_recv.at[0], up).wait_send()
    part = far.at[pl.ds(0, NZ - 1)]
    copy(part, part, far_send, far_recv.at[0], up).wait_send()
    part = pair.at[pl.ds(0, NZ - 2)]
    copy(part, part, pair_send, pair_recv.at[0], up).wait_send()

    way_home = rem(z - rem(col, NZ) + NZ, NZ)
    halved = way_home == NZ - 3
    homes = way_home == 0

    @pl.when(halved)
    def _():
        copy(landing, landing, out_send, out_recv, up).wait_recv()
        out[...] = landing[0] + landing[1]

    @pl.when(homes)
    def _():
        part = landing.at[0, :, pl.ds(0, (RT - 1) * TS)]
        copy(part, part, out_send, out_recv, up).wait_recv()
        part = landing.at[0, :, pl.ds(0, 13 * TS)]
        copy(part, part, out_send, out_recv, up).wait_send()

    @pl.when(jnp.logical_not(homes))
    def _():
        part = landing.at[0, :, pl.ds(0, 14 * TS)]
        copy(part, part, out_send, out_recv, up).wait_send()

    @pl.when(jnp.logical_not(jnp.logical_or(halved, homes)))
    def _():
        copy(landing.at[0], landing.at[0], out_send, out_recv, up).wait_recv()

    @pl.when(jnp.logical_not(halved))
    def _():
        out[...] = landing[0]


def body(tile_values, tile_rows, tile_cols, tile_live, dense_factor):
    dma = pltpu.SemaphoreType.DMA
    vmem = pltpu.VMEM
    f32 = jnp.float32
    return pl.pallas_call(
        kernel,
        out_shape=jax.ShapeDtypeStruct((SHARE, RT * TS), f32),
        in_specs=[pl.BlockSpec(memory_space=pltpu.HBM)] * 5,
        out_specs=pl.BlockSpec(memory_space=pltpu.VMEM),
        scratch_shapes=[
            vmem((NZ, SLOTS, TS, TS), f32),
            vmem((NZ, 3, 1, SLOTS), jnp.int32),
            pltpu.SMEM((NZ, 3, 1, SLOTS), jnp.int32),
            vmem((2, PIECES, SHARE, SPAN), f32),
            vmem((2, SHARE, CT * TS), f32),
            vmem((CT, 4 * SHARE, TS), jnp.bfloat16),
            vmem((NZ, 2, NY, 2, 2 * SHARE, TS), f32),
            vmem((NZ, NY, 2, 2 * SHARE, TS), f32),
            vmem((NZ, 3, 2, 2 * SHARE, TS), f32),
            vmem((NZ, 2 * SHARE, TS), f32),
            vmem((NZ, 2 * SHARE, TS), f32),
            vmem((NY, 2 * SHARE, TS), f32),
            vmem((3, 2 * SHARE, TS), f32),
            vmem((2, SHARE, RT * TS), f32),
            pltpu.SemaphoreType.REGULAR((NZ // 2 - 1, 2)),
            dma((5,)),
            dma, dma((TICKS,)), dma, dma((TICKS,)),
            dma, dma,
            dma((2,)), dma((2, PIECES)), dma((2,)), dma((2,)),
            dma, dma((NZ,)), dma, dma((NZ,)), dma, dma((NZ,)), dma, dma,
            dma, dma, dma, dma, dma,
        ],
        compiler_params=pltpu.CompilerParams(
            collective_id=0, has_side_effects=True, vmem_limit_bytes=56000000
        ),
    )(
        *(
            pltpu.with_memory_space_constraint(value, pltpu.HBM)
            for value in (tile_values[0, 0], tile_rows[0], tile_cols[0], tile_live[0], dense_factor)
        )
    )


def solution(mesh):
    in_specs = (
        P("row", "col", None, None, None),
        P("row", "col", None),
        P("row", "col", None),
        P("row", "col", None),
        P("row", "col"),
    )
    out_specs = P("col", "row")
    return jax.shard_map(body, mesh=mesh, in_specs=in_specs, out_specs=out_specs, check_vma=False)
```
